32 devices in a mesh: seq: 8 (over y, x, core), head: 4 (over z).
Axes of the slice: x: 2, y: 2, z: 4, core: 2. Of those that a mesh axis runs over, the one named last changes fastest.
Arguments:
- tokens: bfloat16 [8192, 2048], P('seq', 'head'), may hold values from -6 to 6
- gain_attn: bfloat16 [2048], P('head'), may hold values from 0.5 to 1.5
- gain_ffn: bfloat16 [2048], P('head'), may hold values from 0.5 to 1.5
- w_query: bfloat16 [2048, 2048], P('seq', 'head'), may hold values from -0.125 to 0.125
- w_key: bfloat16 [2048, 2048], P('seq', 'head'), may hold values from -0.125 to 0.125
- w_value: bfloat16 [2048, 4096], P('seq', 'head'), may hold values from -0.125 to 0.125
- w_gate: bfloat16 [2048, 4096], P('seq', 'head'), may hold values from -0.125 to 0.125
- w_out: bfloat16 [4096, 2048], P('head', 'seq'), may hold values from -0.09375 to 0.09375
- w_up: bfloat16 [2048, 4096], P('seq', 'head'), may hold values from -0.125 to 0.125
- w_down: bfloat16 [4096, 2048], P('head', 'seq'), may hold values from -0.09375 to 0.09375
- log_decay: float32 [8, 8192], P('head', 'seq'), may hold values from -1 to 0
- cotangent: bfloat16 [8192, 2048], P('seq', 'head'), may hold values from -6 to 6
Outputs:
- output: bfloat16 [8192, 2048], P('seq', 'head')
- input_grad: float32 [8192, 2048], P('seq', 'head')
- grad_gain_attn: float32 [2048], P('head')
- grad_gain_ffn: float32 [2048], P('head')
- grad_w_query: float32 [2048, 2048], P('seq', 'head')
- grad_w_key: float32 [2048, 2048], P('seq', 'head')
- grad_w_value: float32 [2048, 4096], P('seq', 'head')
- grad_w_gate: float32 [2048, 4096], P('seq', 'head')
- grad_w_out: float32 [4096, 2048], P('head', 'seq')
- grad_w_up: float32 [2048, 4096], P('seq', 'head')
- grad_w_down: float32 [4096, 2048], P('head', 'seq')
The draws below stay inside these ranges and needn't reach their ends.
All inputs are finite; a program needn't handle non-finite values.
Results may differ from the reference program's by a relative error of at most 0.018.
The reference program's roundings to bfloat16 on the way count: a program that leaves them out, or rounds other values in their place, can miss the bound.
Values may be sent and summed in bfloat16 or wider, within the bound.
A program may use at most 256 MiB of HBM per device.

```python
import math
import jax
import jax.numpy as jnp
from jax import lax

D = 2048
RETENTION_HEADS = 8
DK = 256
DV = 512
FF = 4096
TOK_DEV = 1024
SEQUENCE_TOKENS = 8192


def draw_log_decay(key, part):
    parallel_sequences = jax.random.split(key, 8)
    head_draw = jax.random.uniform(parallel_sequences[0], (RETENTION_HEADS, 1))
    fast_share = 0.5
    slow_floor = 0.2
    fast_heads = head_draw < fast_share
    slow_rate = jnp.exp(jax.random.uniform(parallel_sequences[1], (RETENTION_HEADS, 1), minval=math.log(slow_floor), maxval=math.log(0.5))) / SEQUENCE_TOKENS
    fast_rate = jnp.exp(jax.random.uniform(parallel_sequences[2], (RETENTION_HEADS, 1), minval=math.log(1.0 / 50.0), maxval=math.log(1.0 / 30.0)))
    baseline_decay_rate = jnp.where(fast_heads, fast_rate, slow_rate)
    phases = jax.random.uniform(parallel_sequences[3], (RETENTION_HEADS, 1), minval=0.0, maxval=2.0 * math.pi)
    cycles = jax.random.uniform(parallel_sequences[4], (RETENTION_HEADS, 1), minval=2.0, maxval=4.0)
    position = jnp.arange(SEQUENCE_TOKENS, dtype=jnp.float32)[None, :] / SEQUENCE_TOKENS
    smoothing_amount = jnp.exp(0.7 * jnp.sin(2.0 * math.pi * cycles * position + phases))
    random_perturbation = jnp.exp(jax.random.uniform(parallel_sequences[5], (RETENTION_HEADS, SEQUENCE_TOKENS), minval=math.log(0.5), maxval=math.log(2.0)))
    spike_events = jax.random.uniform(parallel_sequences[6], (RETENTION_HEADS, SEQUENCE_TOKENS)) < 1.5 / SEQUENCE_TOKENS
    dropped_entries = jax.random.uniform(parallel_sequences[7], (RETENTION_HEADS, SEQUENCE_TOKENS), minval=math.log(1.25), maxval=math.log(2.0))
    return -(baseline_decay_rate * smoothing_amount * random_perturbation) - jnp.where(spike_events, dropped_entries, 0.0)


def strengthened(drawn, rng, source, target, parts, factor):
    def block_of(axis_at):
        return (jnp.arange(drawn.shape[axis_at]) // (drawn.shape[axis_at] // parts)).reshape((-1,) + (1,) * (drawn.ndim - 1 - axis_at))

    one_side = jax.random.permutation(rng, parts)[block_of(target)]
    other_side = (block_of(target) + parts // 2) % parts
    return jnp.where((block_of(source) == one_side) | (block_of(source) == other_side), factor * drawn, drawn)


def block_scale(key, dims, pieces, low, top_value):
    loudness = 1.0
    for dim, blocks in pieces:
        steps = jax.random.uniform(jax.random.fold_in(jax.random.fold_in(key, 6), dim), (blocks,), jnp.float32, low / len(pieces), top_value / len(pieces))
        loudness = loudness * jnp.repeat(jnp.exp(steps), dims[dim] // blocks).reshape((-1,) + (1,) * (len(dims) - 1 - dim))
    return loudness


def gaussian(stream_key, dims, scale, most, pieces=(), kind=jnp.bfloat16):
    entries = jax.random.normal(stream_key, dims, jnp.float32) * scale
    if len(pieces) > 0:
        entries = block_scale(stream_key, dims, pieces, -0.22, 0.18) * entries
    return jnp.clip(entries, min=-most, max=most).astype(kind)


def bell_draw_with(stream_key, extent, width, bound, shards, heavy, held_as=jnp.bfloat16):
    values = width * jax.random.normal(stream_key, extent, jnp.float32)
    if shards:
        values = values * block_scale(stream_key, extent, shards, -0.22, 0.18)
    return jnp.clip(strengthened(values, jax.random.fold_in(stream_key, 3), *heavy), -bound, bound).astype(held_as)


def setup_inputs(seed: int = 0) -> dict:
    keys = jax.random.split(jax.random.key(seed), 13)
    return {
        "tokens": gaussian(keys[0], (SEQUENCE_TOKENS, D), 1.0, 6.0, ((0, 8), (1, 4))),
        "gain_attn": jnp.clip(1.0 + 0.1 * jax.random.normal(keys[1], (D,), jnp.float32), 0.5, 1.5).astype(jnp.bfloat16),
        "gain_ffn": jnp.clip(1.0 + 0.1 * jax.random.normal(keys[2], (D,), jnp.float32), 0.5, 1.5).astype(jnp.bfloat16),
        "w_query": gaussian(keys[3], (D, RETENTION_HEADS * DK), D ** -0.5, 0.125, ((0, 8), (1, 4))),
        "w_key": gaussian(keys[4], (D, RETENTION_HEADS * DK), D ** -0.5, 0.125, ((0, 8), (1, 4))),
        "w_value": gaussian(keys[5], (D, RETENTION_HEADS * DV), D ** -0.5, 0.125, ((0, 8), (1, 4))),
        "w_gate": gaussian(keys[6], (D, RETENTION_HEADS * DV), D ** -0.5, 0.125, ((0, 8), (1, 4))),
        "w_out": gaussian(keys[7], (RETENTION_HEADS * DV, D), (RETENTION_HEADS * DV) ** -0.5, 0.09375, ((0, 4), (1, 8))),
        "w_up": gaussian(keys[8], (D, FF), D ** -0.5, 0.125, ((0, 8), (1, 4))),
        "w_down": gaussian(keys[9], (FF, D), FF ** -0.5, 0.09375, ((0, 4), (1, 8))),
        "log_decay": draw_log_decay(jax.random.fold_in(keys[12], 71), 0),
        "cotangent": bell_draw_with(keys[11], (SEQUENCE_TOKENS, D), 1.0, 6.0, ((0, 8), (1, 4)), (0, 1, 8, 2.0)),
    }


exact_precision_mode = lax.Precision.HIGHEST

@jax.custom_vjp
def low(v):
    return lax.optimization_barrier(v.astype(jnp.bfloat16)).astype(jnp.float32)

@jax.custom_vjp
def reduced_precision_backward(v):
    return v

def low_keep(v):
    return (low(v), None)

def low_pass(kept, grad):
    return (grad,)

def back_keep(v):
    return (v, None)

def back_low(kept, grad):
    return (low(grad),)
low.defvjp(low_keep, low_pass)
reduced_precision_backward.defvjp(back_keep, back_low)

def matmul(left, right):
    return jnp.dot(left, right, precision=exact_precision_mode, preferred_element_type=jnp.float32)

def layer_norm(values, gain):
    mean = lax.optimization_barrier(jnp.mean(values, axis=-1, keepdims=True))
    centered = values - mean
    spread = lax.optimization_barrier(jnp.mean(centered * centered, axis=-1, keepdims=True))
    return centered * lax.rsqrt(spread + 1e-05) * gain

def group_norm(values):
    mean = lax.optimization_barrier(jnp.mean(values, axis=-1, keepdims=True))
    centered = values - mean
    spread = lax.optimization_barrier(jnp.mean(centered * centered, axis=-1, keepdims=True))
    return centered * lax.rsqrt(spread + 1e-05)

def retain_block(state, block):
    query_matrix_rows, key_matrix_rows, value_matrix_rows, decay_rows = block
    running = jnp.cumsum(decay_rows, axis=1)
    block_decay = running[:, -1]
    span = running.shape[1]
    gap = running[:, :, None] - running[:, None, :]
    lower = jnp.arange(span)[:, None] >= jnp.arange(span)[None, :]
    weights_in = jnp.where(lower[None], jnp.exp(jnp.minimum(gap, 0.0)), 0.0)
    unscaled_scores = reduced_precision_backward(jnp.einsum('gqz,wqz->qgw', query_matrix_rows, key_matrix_rows, precision=exact_precision_mode))
    weighted = low(unscaled_scores * weights_in)
    query_scale = jnp.exp(running).T[:, :, None]
    key_scaling_factor = jnp.exp(block_decay[:, None] - running).T[:, :, None]
    query_decay = low(query_matrix_rows * query_scale)
    key_decay_factors = low(key_matrix_rows * key_scaling_factor)
    local_retention_state = reduced_precision_backward(jnp.einsum('gct,gcx->ctx', key_decay_factors, value_matrix_rows, precision=exact_precision_mode))
    intra = jnp.einsum('hnm,mhe->nhe', weighted, value_matrix_rows, precision=exact_precision_mode)
    inter = jnp.einsum('nhd,hde->nhe', query_decay, low(state), precision=exact_precision_mode)
    new_state = jnp.exp(block_decay)[:, None, None] * state + local_retention_state
    return (new_state, intra + inter)

def forward(tokens, gain_attn, gain_ffn, w_query, w_key, w_value, w_gate, w_out, w_up, w_down, log_decay):
    normed = low(layer_norm(tokens, gain_attn))
    query_matrix_rows = reduced_precision_backward(low(matmul(normed, w_query)))
    key_matrix_rows = reduced_precision_backward(low(matmul(normed, w_key)))
    value_matrix_rows = reduced_precision_backward(low(matmul(normed, w_value)))
    gate_pre = reduced_precision_backward(matmul(normed, w_gate))
    block_count = SEQUENCE_TOKENS // TOK_DEV
    split_query = query_matrix_rows.reshape(block_count, TOK_DEV, RETENTION_HEADS, DK)
    split_key = key_matrix_rows.reshape(block_count, TOK_DEV, RETENTION_HEADS, DK)
    split_value = value_matrix_rows.reshape(block_count, TOK_DEV, RETENTION_HEADS, DV)
    split_decay = log_decay.reshape(RETENTION_HEADS, block_count, TOK_DEV).transpose(1, 0, 2)
    initial = jnp.zeros((RETENTION_HEADS, DK, DV), jnp.float32)
    _, retained = lax.scan(jax.checkpoint(retain_block), initial, (split_query, split_key, split_value, split_decay))
    retained = reduced_precision_backward(retained.reshape(SEQUENCE_TOKENS, RETENTION_HEADS, DV))
    grouped = group_norm(retained).reshape(SEQUENCE_TOKENS, RETENTION_HEADS * DV)
    mixed_rows = low(jax.nn.silu(gate_pre) * grouped)
    attended = reduced_precision_backward(matmul(mixed_rows, w_out))
    hidden = tokens + attended
    normed_ffn = low(layer_norm(low(hidden), gain_ffn))
    pre_act = reduced_precision_backward(matmul(normed_ffn, w_up))
    activated = low(jax.nn.gelu(pre_act, approximate=True))
    return hidden + matmul(activated, w_down)

def reference(tokens, gain_attn, gain_ffn, w_query, w_key, w_value, w_gate, w_out, w_up, w_down, log_decay, cotangent):

    def wrapped(tok_in, gain_one, gain_two, query_w, key_w, value_w, gate_w, out_w, up_w, down_w):
        return forward(tok_in, gain_one, gain_two, query_w, key_w, value_w, gate_w, out_w, up_w, down_w, log_decay)
    result, pull_back = jax.vjp(wrapped, tokens.astype(jnp.float32), gain_attn.astype(jnp.float32), gain_ffn.astype(jnp.float32), w_query.astype(jnp.float32), w_key.astype(jnp.float32), w_value.astype(jnp.float32), w_gate.astype(jnp.float32), w_out.astype(jnp.float32), w_up.astype(jnp.float32), w_down.astype(jnp.float32))
    grads = pull_back(cotangent.astype(jnp.float32))
    return (result.astype(jnp.bfloat16), grads[0], grads[1], grads[2], grads[3], grads[4], grads[5], grads[6], grads[7], grads[8], grads[9])
```

```python
import jax
import jax.numpy as jnp
from jax import lax
from jax.sharding import Mesh
from jax.sharding import PartitionSpec as P

F32 = jnp.float32
BF16 = jnp.bfloat16

SWAP = ((0, 0), (1, 2), (2, 1), (3, 3))
MOVE = ((0, 1), (1, 3), (2, 0), (3, 2))
BACK = ((1, 0), (3, 1), (0, 2), (2, 3))
FLIP = ((0, 1), (1, 0))


def swap(v):
    return lax.ppermute(v, ("c", "zh"), SWAP)


def ordered(first, second, flag, axis):
    return jnp.where(
        flag == 0,
        jnp.concatenate([first, second], axis),
        jnp.concatenate([second, first], axis),
    )


def gather_group(v):
    near = ordered(v, lax.ppermute(v, "zl", FLIP), lax.axis_index("zl"), 1)
    return ordered(near, lax.ppermute(near, "c", FLIP), lax.axis_index("c"), 1)


def half(v, which):
    size = v.shape[1] // 2
    return lax.dynamic_slice_in_dim(v, which * size, size, 1)


def scatter_group(v):
    c, zl = lax.axis_index("c"), lax.axis_index("zl")
    far = lax.ppermute(half(v, 1 - c).astype(BF16), "c", FLIP)
    v = half(v, c) + far.astype(F32)
    far = lax.ppermute(half(v, 1 - zl).astype(BF16), "zl", FLIP)
    return half(v, zl) + far.astype(F32)


def sum_group(v):
    v = v + lax.ppermute(v, "c", FLIP)
    return v + lax.ppermute(v, "zl", FLIP)


def gather_weight(w, axis):
    moved = lax.ppermute(w, ("c", "zh"), MOVE)
    swapped = swap(w)
    pair = ordered(swapped, moved, lax.axis_index("zh"), axis)
    return lax.all_gather(pair, "p", axis=axis, tiled=True)


def scatter_weight(g, axis):
    part = lax.psum_scatter(g.astype(BF16), "p", scatter_dimension=axis, tiled=True)
    zh = lax.axis_index("zh")
    size = part.shape[axis] // 2
    moved = lax.dynamic_slice_in_dim(part, (1 - zh) * size, size, axis)
    swapped = lax.dynamic_slice_in_dim(part, zh * size, size, axis)
    moved = lax.ppermute(moved, ("c", "zh"), BACK)
    return moved.astype(F32) + swap(swapped).astype(F32)


def moments(values):
    mean = jnp.mean(values, axis=-1, keepdims=True)
    centered = values - mean
    spread = jnp.mean(centered * centered, axis=-1, keepdims=True)
    return mean, lax.rsqrt(spread + 1e-05)


def group_norm(values):
    mean, scale = moments(values)
    return (values - mean) * scale


def gelu_tanh(values):
    return jax.nn.gelu(values, approximate=True)


def gated(gate_pre, grouped):
    return jax.nn.silu(gate_pre) * grouped


def decay_weights(running):
    span = running.shape[1]
    gap = running[:, :, None] - running[:, None, :]
    lower = jnp.arange(span)[:, None] >= jnp.arange(span)[None, :]
    return jnp.where(lower[None], jnp.exp(jnp.minimum(gap, 0.0)), 0.0)


def dot(a, b, dims):
    return lax.dot_general(a, b, (dims, ((), ())), preferred_element_type=F32)


def norm_back(d, low, mean, scale, gain, width):
    hat = (low.astype(F32) - mean) * scale
    scaled = d * gain
    sums = sum_group(jnp.stack([jnp.sum(scaled, 1), jnp.sum(scaled * hat, 1)])) / width
    d_in = scale * (scaled - sums[0][:, None] - hat * sums[1][:, None])
    return d_in, jnp.sum(d * hat, 0)


def on_device(
    tokens,
    gain_attn,
    gain_ffn,
    w_query,
    w_key,
    w_value,
    w_gate,
    w_out,
    w_up,
    w_down,
    log_decay,
    cotangent,
):
    rows = tokens.shape[0]
    heads = log_decay.shape[0]
    cols = tokens.shape[1]
    quarter = 2 * lax.axis_index("c") + lax.axis_index("zl")
    block = 2 * lax.axis_index("p") + lax.axis_index("zh")
    blocks = 2 * lax.axis_size("p")

    sums_here = jnp.sum(log_decay, axis=1)
    block_sums = swap(lax.all_gather(sums_here, ("p", "c"), axis=0))
    tokens_own = swap(tokens)
    log_decay = swap(log_decay)
    gains = lax.all_gather(jnp.stack([gain_attn, gain_ffn]), ("zh", "zl"), axis=1, tiled=True)
    gain_one, gain_two = gains[0].astype(F32), gains[1].astype(F32)
    full_query = gather_weight(w_query, 0)
    rows_full = gather_group(tokens_own)
    full_key = gather_weight(w_key, 0)
    full_value = gather_weight(w_value, 0)
    full_gate = gather_weight(w_gate, 0)
    full_out = gather_weight(w_out, 1)
    full_up = gather_weight(w_up, 0)
    full_down = gather_weight(w_down, 1)
    grad_own = swap(cotangent)
    grad_full = gather_group(grad_own)
    width = rows_full.shape[1]
    key_width = full_query.shape[1] // heads
    value_width = full_value.shape[1] // heads
    gain_one_own = lax.dynamic_slice_in_dim(gain_one, quarter * cols, cols, 0)
    gain_two_own = lax.dynamic_slice_in_dim(gain_two, quarter * cols, cols, 0)

    place = jnp.arange(blocks)
    total = jnp.cumsum(block_sums, axis=0)
    before = total - block_sums
    at_block = lax.dynamic_index_in_dim(before, block, 0, False)
    to_block = lax.dynamic_index_in_dim(total, block, 0, False)
    earlier = jnp.where(
        (place < block)[:, None], jnp.exp(jnp.minimum(at_block[None] - total, 0.0)), 0.0
    )
    later = jnp.where(
        (place > block)[:, None], jnp.exp(jnp.minimum(before - to_block[None], 0.0)), 0.0
    )

    mean_one, scale_one = moments(rows_full.astype(F32))
    normed = ((rows_full.astype(F32) - mean_one) * scale_one * gain_one).astype(BF16)
    nn = ((1,), (0,))
    nt = ((1,), (1,))
    tn = ((0,), (0,))
    query_rows = dot(normed, full_query, nn).astype(BF16).reshape(rows, heads, key_width)
    key_rows = dot(normed, full_key, nn).astype(BF16).reshape(rows, heads, key_width)
    value_rows = dot(normed, full_value, nn).astype(BF16).reshape(rows, heads, value_width)
    gate_pre = dot(normed, full_gate, nn)
    running = jnp.cumsum(log_decay, axis=1)
    block_decay = running[:, -1]
    query_scale = jnp.exp(running).T[:, :, None]
    key_scale = jnp.exp(block_decay[:, None] - running).T[:, :, None]
    key_decay = (key_rows * key_scale).astype(BF16)
    query_decay = (query_rows * query_scale).astype(BF16)

    def einsum(spec, a, b):
        return jnp.einsum(spec, a, b, preferred_element_type=F32)

    def carried(part, weights):
        every = lax.all_gather(part.astype(BF16), ("p", "zh"), axis=0)
        return jnp.sum(every.astype(F32) * weights[:, :, None, None], axis=0).astype(BF16)

    state = carried(einsum("nhd,nhe->hde", key_decay, value_rows), earlier)
    decays = decay_weights(running)
    weighted = (einsum("nhd,mhd->hnm", query_rows, key_rows) * decays).astype(BF16)
    retained = einsum("hnm,mhe->nhe", weighted, value_rows) + einsum(
        "nhd,hde->nhe", query_decay, state
    )
    grouped = group_norm(retained).reshape(rows, heads * value_width)
    mixed_rows = gated(gate_pre, grouped).astype(BF16)
    attended = scatter_group(dot(mixed_rows, full_out, nn))
    hidden = tokens_own.astype(F32) + attended
    hidden_own = hidden.astype(BF16)
    hidden_full = gather_group(hidden_own).astype(F32)
    mean_two, scale_two = moments(hidden_full)
    normed_ffn = ((hidden_full - mean_two) * scale_two * gain_two).astype(BF16)
    pre_act = dot(normed_ffn, full_up, nn)
    activated, gelu_back = jax.vjp(gelu_tanh, pre_act)
    activated = activated.astype(BF16)
    d_act = dot(grad_full, full_down, nt)
    d_pre = gelu_back(d_act)[0].astype(BF16)
    d_normed_ffn = scatter_group(dot(d_pre, full_up, nt))
    output = swap((hidden + scatter_group(dot(activated, full_down, nn))).astype(BF16))
    grad_down = scatter_weight(dot(activated, grad_full, tn), 1)
    grad_up = scatter_weight(dot(normed_ffn, d_pre, tn), 0)
    d_hidden_norm, d_gain_two = norm_back(
        d_normed_ffn, hidden_own, mean_two, scale_two, gain_two_own, width
    )
    d_hidden = grad_own.astype(F32) + d_hidden_norm
    d_attended = gather_group(d_hidden.astype(BF16))
    grad_out = scatter_weight(dot(mixed_rows, d_attended, tn), 1)
    d_mixed = dot(d_attended, full_out, nt)
    _, gate_back = jax.vjp(gated, gate_pre, grouped)
    d_gate, d_grouped = gate_back(d_mixed)
    d_gate = d_gate.astype(BF16)
    grad_gate = scatter_weight(dot(normed, d_gate, tn), 0)
    _, group_back = jax.vjp(group_norm, retained)
    d_retained = group_back(d_grouped.reshape(rows, heads, value_width))[0].astype(BF16)
    later_grad = carried(einsum("nhd,nhe->hde", query_decay, d_retained), later)
    d_raw = (einsum("nhe,mhe->hnm", d_retained, value_rows) * decays).astype(BF16)
    d_query = (
        einsum("hnm,mhd->nhd", d_raw, key_rows)
        + einsum("nhe,hde->nhd", d_retained, state) * query_scale
    )
    d_query = d_query.astype(BF16).reshape(rows, heads * key_width)
    d_keys = (
        einsum("hnm,nhd->mhd", d_raw, query_rows)
        + einsum("mhe,hde->mhd", value_rows, later_grad) * key_scale
    )
    d_keys = d_keys.astype(BF16).reshape(rows, heads * key_width)
    d_values = einsum("hnm,nhe->mhe", weighted, d_retained) + einsum(
        "mhd,hde->mhe", key_decay, later_grad
    )
    d_values = d_values.astype(BF16).reshape(rows, heads * value_width)
    grad_value = scatter_weight(dot(normed, d_values, tn), 0)
    grad_key = scatter_weight(dot(normed, d_keys, tn), 0)
    grad_query = scatter_weight(dot(normed, d_query, tn), 0)
    d_normed = scatter_group(
        dot(d_gate, full_gate, nt)
        + dot(d_query, full_query, nt)
        + dot(d_keys, full_key, nt)
        + dot(d_values, full_value, nt)
    )
    d_tokens_norm, d_gain_one = norm_back(
        d_normed, tokens_own, mean_one, scale_one, gain_one_own, width
    )
    input_grad = swap((d_hidden + d_tokens_norm).astype(BF16)).astype(F32)
    gain_sums = swap(lax.psum(jnp.stack([d_gain_one, d_gain_two]), ("p", "zh")))
    return (
        output,
        input_grad,
        gain_sums[0],
        gain_sums[1],
        grad_query,
        grad_key,
        grad_value,
        grad_gate,
        grad_out,
        grad_up,
        grad_down,
    )


def solution(mesh):
    seq, head = mesh.devices.shape
    finer = Mesh(mesh.devices.reshape(seq // 2, 2, head // 2, 2), ("p", "c", "zh", "zl"))
    seq, head = ("p", "c"), ("zh", "zl")
    by_row, by_column, one = P(seq, head), P(head, seq), P(head)
    in_specs = (
        (by_row, one, one) + (by_row,) * 4 + (by_column, by_row, by_column) + (by_column, by_row)
    )
    out_specs = (by_row, by_row, one, one) + (by_row,) * 4 + (by_column, by_row, by_column)
    return jax.shard_map(
        on_device, mesh=finer, in_specs=in_specs, out_specs=out_specs, check_vma=False
    )
```

```python
import functools

import jax
import jax.numpy as jnp
from jax import lax
from jax.experimental import pallas as pl
from jax.experimental.pallas import tpu as pltpu
from jax.sharding import Mesh
from jax.sharding import PartitionSpec as P

F32 = jnp.float32
BF16 = jnp.bfloat16

SWAP = ((0, 0), (1, 2), (2, 1), (3, 3))
MOVE = ((0, 1), (1, 3), (2, 0), (3, 2))
BACK = ((1, 0), (3, 1), (0, 2), (2, 3))
FLIP = ((0, 1), (1, 0))


def moments(values):
    mean = jnp.mean(values, axis=-1, keepdims=True)
    centered = values - mean
    spread = jnp.mean(centered * centered, axis=-1, keepdims=True)
    return mean, lax.rsqrt(spread + 1e-05)


MESH = pl.DeviceIdType.MESH


def bits_of(count):
    return count.bit_length() - 1


def flipped(index, stride):
    return index + stride * (1 - 2 * lax.rem(lax.div(index, stride), 2))


class Place:
    def __init__(self, chips):
        self.p, self.c = lax.axis_index("p"), lax.axis_index("c")
        self.zh, self.zl = lax.axis_index("zh"), lax.axis_index("zl")
        self.bits = bits_of(chips)
        self.crossed = lax.rem(self.c + self.zh, 2)
        self.core = {"c": 1 - self.c}
        self.high = {"zh": 1 - self.zh}
        self.diagonal = {"c": 1 - self.c, "zh": 1 - self.zh}
        self.low = {"zl": 1 - self.zl}

    def chip(self, bit):
        return {"p": flipped(self.p, 2**bit)}

    def meet(self):
        barrier = pltpu.get_barrier_semaphore()
        partners = [self.core, self.high, self.diagonal, self.low]
        partners += [self.chip(bit) for bit in range(self.bits)]
        for partner in partners:
            pl.semaphore_signal(barrier, inc=1, device_id=partner, device_id_type=MESH)
        pl.semaphore_wait(barrier, len(partners))

    def moved_to(self):
        return {
            "c": self.c + self.crossed * (1 - 2 * self.c),
            "zh": self.zh + (1 - self.crossed) * (1 - 2 * self.zh),
        }


def remote(src, dst, send, recv, device):
    return pltpu.make_async_remote_copy(
        src_ref=src,
        dst_ref=dst,
        send_sem=send,
        recv_sem=recv,
        device_id=device,
        device_id_type=MESH,
    )


class Relabel:
    def __init__(self, place, src, dst, send, recv):
        self.place = place
        self.moved = remote(src, dst, send.at[0], recv.at[0], place.moved_to())
        self.swapped = remote(src, dst, send.at[1], recv.at[1], place.diagonal)
        self.kept = pltpu.make_async_copy(src, dst, recv.at[1])

    def start(self):
        self.moved.start()
        pl.when(self.place.crossed == 1)(self.swapped.start)
        pl.when(self.place.crossed == 0)(self.kept.start)

    def arrive(self):
        self.moved.wait_recv()
        pl.when(self.place.crossed == 1)(self.swapped.wait_recv)
        pl.when(self.place.crossed == 0)(self.kept.wait)

    def finish(self):
        self.moved.wait_send()
        pl.when(self.place.crossed == 1)(self.swapped.wait_send)


class Spread:
    def __init__(self, place, dst, send, recv):
        self.place, self.dst, self.send, self.recv = place, dst, send, recv
        self.orders = [list(range(place.bits)), list(reversed(range(place.bits)))]

    def copy(self, h, step, mask):
        order = self.orders[h]
        block = self.place.p
        for at in range(self.place.bits):
            if mask >> at & 1:
                block = flipped(block, 2 ** order[at])
        ref = self.dst.at[2 * block + h]
        name = mask + 2**step
        return remote(ref, ref, self.send.at[h, name], self.recv.at[h, name], self.place.chip(order[step]))

    def start(self):
        for step in range(self.place.bits):
            for h in range(2):
                self.copy(h, step, 0).start()

    def arrive(self, mask):
        for h in range(2):
            top = bits_of(mask)
            self.copy(h, top, mask - 2**top).wait_recv()
            for step in range(top + 1, self.place.bits):
                self.copy(h, step, mask).start()

    def rest(self, since):
        for mask in range(since, 2**self.place.bits):
            self.arrive(mask)

    def finish(self):
        for h in range(2):
            for mask in range(1, 2**self.place.bits):
                top = bits_of(mask)
                self.copy(h, top, mask - 2**top).wait_send()


class Columns:
    def __init__(self, place, src, full, send, recv):
        self.place = place
        cols = src.shape[1]

        def at(zl, c):
            return full.at[:, pl.ds(pl.multiple_of((2 * c + zl) * cols, cols), cols)]

        own, near = at(place.zl, place.c), at(1 - place.zl, place.c)
        self.own = own
        crossing = at(place.zl, 1 - place.c)
        self.swapped = remote(src, crossing, send.at[0], recv.at[0], place.diagonal)
        self.kept = pltpu.make_async_copy(src, own, recv.at[0])
        self.low = remote(own, own, send.at[1], recv.at[1], place.low)
        self.core = remote(own, own, send.at[2], recv.at[2], place.core)
        self.passed = remote(near, near, send.at[3], recv.at[3], place.core)

    def start(self):
        pl.when(self.place.crossed == 1)(self.swapped.start)
        pl.when(self.place.crossed == 0)(self.kept.start)

    def second(self):
        pl.when(self.place.crossed == 1)(self.swapped.wait_recv)
        pl.when(self.place.crossed == 0)(self.kept.wait)
        self.low.start()
        self.core.start()

    def third(self):
        self.low.wait_recv()
        self.passed.start()

    def finish(self):
        pl.when(self.place.crossed == 1)(self.swapped.wait_send)
        self.low.wait_send()
        self.core.wait_send()
        self.passed.wait_send()


def project_kernel(chips, *refs):
    decay, query, key, value, gate, out, tokens, cotangent = refs[:8]
    results = refs[8:24]
    full_decay, full_query, full_key, full_value, full_gate, full_out = results[:6]
    grad_full, tokens_own, grad_own, gains, normed, query_rows = results[6:12]
    key_rows, value_rows, gate_pre, stats = results[12:]
    every, weight, zsend, zrecv, send, recv, tsend, trecv, local = refs[24:]
    place = Place(chips)
    place.meet()
    shards = [decay, query, key, value, gate, out]
    fulls = [full_decay, full_query, full_key, full_value, full_gate, full_out]
    labels = [Relabel(place, s, f.at[2 * place.p + place.c], zsend.at[i], zrecv.at[i]) for i, (s, f) in enumerate(zip(shards, fulls))]
    spreads = [Spread(place, f, send.at[i], recv.at[i]) for i, f in enumerate(fulls)]
    held = Columns(place, tokens, every, tsend.at[0], trecv.at[0])
    grads = Columns(place, cotangent, grad_full, tsend.at[1], trecv.at[1])
    for i in range(4):
        labels[i].start()
    held.start()

    def spread(i):
        labels[i].arrive()
        spreads[i].start()

    count = tokens.shape[0] - 16
    tile = min(128, count)

    def norm():
        gain = every[count : count + 1, :].astype(F32)

        def one(i, carry):
            at = pl.ds(pl.multiple_of(i * tile, tile), tile)
            v = every[at, :].astype(F32)
            mean, scale = moments(v)
            normed[at, :] = ((v - mean) * scale * gain).astype(BF16)
            stats[0, at, :] = jnp.broadcast_to(mean, (tile, 128))
            stats[1, at, :] = jnp.broadcast_to(scale, (tile, 128))
            return carry

        lax.fori_loop(0, count // tile, one, 0)

    step = min(256, count)

    def project(i, rows):
        spreads[i].rest(2)
        full = fulls[i]
        slots, height, columns = full.shape
        held_weight = weight.at[:, :, pl.ds(0, columns)]
        copy = pltpu.make_async_copy(full, held_weight, local.at[0])
        copy.start()
        copy.wait()

        def one(j, carry):
            at = pl.ds(pl.multiple_of(j * step, step), step)
            w = held_weight[...].reshape(slots * height, columns)
            v = jnp.dot(normed[at, :], w, preferred_element_type=F32)
            rows[at, :] = v.astype(rows.dtype)
            return carry

        lax.fori_loop(0, count // step, one, 0)

    spread(0)
    spread(1)
    spread(2)
    spreads[0].arrive(1)
    spreads[1].arrive(1)
    spread(3)
    spreads[2].arrive(1)
    held.second()
    held.core.wait_recv()
    labels[4].start()
    labels[5].start()
    grads.start()
    spreads[3].arrive(1)
    held.third()
    spread(4)
    held.passed.wait_recv()
    norm()
    project(1, query_rows)
    project(2, key_rows)
    spread(5)
    spreads[4].arrive(1)
    project(3, value_rows)
    grads.second()
    spreads[5].arrive(1)
    project(4, gate_pre)
    grads.third()
    spreads[0].rest(2)
    grads.core.wait_recv()
    grads.passed.wait_recv()
    spreads[5].rest(2)
    keep = [
        pltpu.make_async_copy(held.own, tokens_own, local.at[1]),
        pltpu.make_async_copy(every.at[pl.ds(count, 16)], gains, local.at[2]),
        pltpu.make_async_copy(grads.own, grad_own, local.at[3]),
    ]
    for copy in keep:
        copy.start()
    for i in range(6):
        labels[i].finish()
        spreads[i].finish()
    held.finish()
    grads.finish()
    for copy in keep:
        copy.wait()


def gather_and_project(chips, decay, query, key, value, gate, out, tokens, cotangent):
    shards = [decay, query, key, value, gate, out]
    rows, cols = tokens.shape[0] - 16, tokens.shape[1]
    width = 4 * cols
    slots = 2 * chips
    shape = jax.ShapeDtypeStruct
    vmem = pl.BlockSpec(memory_space=pltpu.VMEM)
    hbm = pl.BlockSpec(memory_space=pl.ANY)
    gathered = [shape((slots, *s.shape), s.dtype) for s in shards]
    wide = [query.shape[1], key.shape[1], value.shape[1], gate.shape[1]]
    made = [
        shape((rows, width), BF16),
        shape((tokens.shape[0], cols), BF16),
        shape((rows, cols), BF16),
        shape((16, width), BF16),
        shape((rows, width), BF16),
        shape((rows, wide[0]), BF16),
        shape((rows, wide[1]), BF16),
        shape((rows, wide[2]), BF16),
        shape((rows, wide[3]), F32),
        shape((2, rows, 128), F32),
    ]
    names = 2 ** bits_of(chips)
    dma = pltpu.SemaphoreType.DMA
    flops = 2 * rows * width * sum(wide)
    return pl.pallas_call(
        functools.partial(project_kernel, chips),
        out_shape=gathered + made,
        in_specs=[vmem] * 8,
        out_specs=[hbm] * 10 + [vmem] * 6,
        scratch_shapes=[
            pltpu.VMEM((tokens.shape[0], width), BF16),
            pltpu.VMEM((slots, value.shape[0], value.shape[1]), BF16),
            dma((6, 2)),
            dma((6, 2)),
            dma((6, 2, names)),
            dma((6, 2, names)),
            dma((2, 4)),
            dma((2, 4)),
            dma((4,)),
        ],
        compiler_params=pltpu.CompilerParams(
            collective_id=0, has_side_effects=True, vmem_limit_bytes=60 * 2**20
        ),
        cost_estimate=pl.CostEstimate(flops=flops, bytes_accessed=60 * 2**20, transcendentals=0),
        name="gather_project",
    )(*shards, tokens, cotangent)


def reduce_kernel(chips, count, ready_count, swap_count, gains, *refs):
    refs = list(refs)

    def taken(number):
        front = refs[:number]
        del refs[:number]
        return front

    (turned,) = taken(1)
    grads, ready, swaps, gain = taken(count), taken(ready_count), taken(swap_count), taken(gains)
    results, totals, swapped_to = taken(count), taken(ready_count), taken(swap_count)
    gain_to = taken(gains)
    parts, arrived, handed = taken(count), taken(count), taken(count)
    ready_handed = taken(ready_count)
    send, recv, zsend, zrecv = taken(4)
    place = Place(chips)
    place.meet()
    bits = place.bits
    orders = [list(range(bits)), list(reversed(range(bits)))]
    back = {
        "c": place.c + (1 - place.crossed) * (1 - 2 * place.c),
        "zh": place.zh + place.crossed * (1 - 2 * place.zh),
    }

    def slot(h, mask):
        block = place.p
        for at in range(bits):
            if mask >> at & 1:
                block = flipped(block, 2 ** orders[h][at])
        return 2 * block + h

    def added(target, first, second):
        height = first.shape[0]
        step = min(64, height)

        def one(i, carry):
            at = pl.ds(pl.multiple_of(i * step, step), step)
            v = first[at, :].astype(F32) + second[at, :].astype(F32)
            target[at, :] = v.astype(target.dtype)
            return carry

        lax.fori_loop(0, height // step, one, 0)

    def hop(i, h, step, mask):
        name = mask + 2**step
        return remote(
            parts[i].at[slot(h, name)],
            arrived[i].at[h, name],
            send.at[i, h, name],
            recv.at[i, h, name],
            place.chip(orders[h][step]),
        )

    def give(i, step):
        for mask in reversed(range(2**step)):
            for h in range(2):
                hop(i, h, step, mask).start()

    def take(i, step):
        for mask in reversed(range(2**step)):
            for h in range(2):
                hop(i, h, step, mask).wait_recv()
                mine = parts[i].at[slot(h, mask)]
                added(mine, mine, arrived[i].at[h, 2**step + mask])

    def hand(i):
        if i < count:
            even, odd, to = parts[i].at[2 * place.p + 1 - place.zh], own(i), handed[i]
        else:
            even, odd, to = ready[i - count].at[1 - place.zh], own(i), ready_handed[i - count]
        moved = remote(even, to.at[0], zsend.at[i, 0], zrecv.at[i, 0], back)
        swapped = remote(odd, to.at[1], zsend.at[i, 1], zrecv.at[i, 1], place.diagonal)
        return moved, swapped

    def own(i):
        if i < count:
            return parts[i].at[2 * place.p + place.zh]
        return ready[i - count].at[place.zh]

    def hand_out(i):
        moved, swapped = hand(i)
        moved.start()
        pl.when(place.crossed == 1)(swapped.start)

    def settle(i):
        to = handed[i] if i < count else ready_handed[i - count]
        result = results[i] if i < count else totals[i - count]
        moved, swapped = hand(i)
        moved.wait_recv()

        @pl.when(place.crossed == 1)
        def _():
            swapped.wait_recv()
            added(result, to.at[0], to.at[1])

        @pl.when(place.crossed == 0)
        def _():
            added(result, to.at[0], own(i))

    def swapping(i):
        src, dst = swaps[i], swapped_to[i]
        at = count + ready_count + i
        over = remote(src, dst, zsend.at[at, 0], zrecv.at[at, 0], place.diagonal)
        return over, pltpu.make_async_copy(src, dst, zrecv.at[at, 0])

    def multiply(i):
        slots, height, _ = parts[i].shape

        def one(s, carry):
            at = pl.ds(pl.multiple_of(s * height, height), height)
            v = jnp.dot(turned[at, :], grads[i][...], preferred_element_type=F32)
            parts[i][s] = v.astype(BF16)
            return carry

        lax.fori_loop(0, slots, one, 0)

    def stage(i, at):
        if at == 0:
            multiply(i)
            give(i, bits - 1)
        elif at < bits:
            take(i, bits - at)
            give(i, bits - at - 1)
        elif at == bits:
            take(i, 0)
            hand_out(i)
        else:
            settle(i)

    for i in range(ready_count):
        hand_out(count + i)
    for i in range(swap_count):
        over, kept = swapping(i)
        pl.when(place.crossed == 1)(over.start)
        pl.when(place.crossed == 0)(kept.start)
    if gains:
        steps, landed, gsend, grecv = taken(4)
        partners = [place.high] + [place.chip(bit) for bit in range(bits)]

        def step(k):
            return remote(steps.at[k], landed.at[k], gsend.at[k], grecv.at[k], partners[k])

        over = remote(steps.at[bits + 1], gain_to[0], gsend.at[bits + 1], grecv.at[bits + 1], place.diagonal)
        kept = pltpu.make_async_copy(steps.at[bits + 1], gain_to[0], grecv.at[bits + 1])
        steps[0] = gain[0][...]
        step(0).start()
    for tick in range(count + bits + 1):
        for at in range(bits + 2):
            if 0 <= tick - at < count:
                stage(tick - at, at)
    if gains:
        for k in range(bits + 1):
            step(k).wait_recv()
            steps[k + 1] = steps[k] + landed[k]
            if k < bits:
                step(k + 1).start()
        pl.when(place.crossed == 1)(over.start)
        pl.when(place.crossed == 0)(kept.start)
    for i in range(ready_count):
        settle(count + i)
    for i in range(count):
        for h in range(2):
            for at in range(bits):
                for mask in range(2**at):
                    hop(i, h, at, mask).wait_send()
    for i in range(count + ready_count):
        moved, swapped = hand(i)
        moved.wait_send()
        pl.when(place.crossed == 1)(swapped.wait_send)
    if gains:
        for k in range(bits + 1):
            step(k).wait_send()
        pl.when(place.crossed == 1)(over.wait)
        pl.when(place.crossed == 0)(kept.wait)
    for i in range(swap_count):
        over, kept = swapping(i)
        pl.when(place.crossed == 1)(over.wait)
        pl.when(place.crossed == 0)(kept.wait)


def reduce_gradients(chips, identity, turned, grads, ready=(), swaps=(), gain=()):
    count = len(grads)
    width, rows = turned.shape
    slots = 2 * chips
    height = width // slots
    vmem = pl.BlockSpec(memory_space=pltpu.VMEM)
    wide = [g.shape[1] for g in grads]
    shape = jax.ShapeDtypeStruct
    dma = pltpu.SemaphoreType.DMA
    moves = count + len(ready) + len(swaps)
    hops = bits_of(chips) + 2
    extra = []
    if gain:
        extra = [pltpu.VMEM((hops, *gain[0].shape), F32)] * 2 + [dma((hops,)), dma((hops,))]
    results = pl.pallas_call(
        functools.partial(reduce_kernel, chips, count, len(ready), len(swaps), len(gain)),
        out_shape=[shape((height, w), F32) for w in wide]
        + [shape(r.shape[1:], F32) for r in ready]
        + [shape(v.shape, v.dtype) for v in (*swaps, *gain)],
        in_specs=[vmem] * (1 + moves + len(gain)),
        out_specs=[vmem] * (moves + len(gain)),
        scratch_shapes=[pltpu.VMEM((slots, height, w), BF16) for w in wide]
        + [pltpu.VMEM((2, chips, height, w), BF16) for w in wide]
        + [pltpu.VMEM((2, height, w), BF16) for w in wide]
        + [pltpu.VMEM(r.shape, BF16) for r in ready]
        + [dma((count, 2, chips)), dma((count, 2, chips)), dma((moves, 2)), dma((moves, 2))]
        + extra,
        compiler_params=pltpu.CompilerParams(
            collective_id=identity, has_side_effects=True, vmem_limit_bytes=60 * 2**20
        ),
        cost_estimate=pl.CostEstimate(
            flops=2 * rows * width * sum(wide), bytes_accessed=60 * 2**20, transcendentals=0
        ),
        name=f"reduce_gradients_{identity}",
    )(turned, *grads, *ready, *swaps, *gain)
    return results


def swap(v):
    return lax.ppermute(v, ("c", "zh"), SWAP)


def ordered(first, second, flag, axis):
    return jnp.where(
        flag == 0,
        jnp.concatenate([first, second], axis),
        jnp.concatenate([second, first], axis),
    )


def gather_group(v, fill=()):
    far, fill = lax.optimization_barrier((lax.ppermute(v, "zl", FLIP), fill))
    near = ordered(v, far, lax.axis_index("zl"), 1)
    return ordered(near, lax.ppermute(near, "c", FLIP), lax.axis_index("c"), 1), fill


def half(v, which):
    size = v.shape[1] // 2
    return lax.dynamic_slice_in_dim(v, which * size, size, 1)


def scatter_group(v, fill=()):
    c, zl = lax.axis_index("c"), lax.axis_index("zl")
    far = lax.ppermute(half(v, 1 - c).astype(BF16), "c", FLIP)
    v = half(v, c) + far.astype(F32)
    far = lax.ppermute(half(v, 1 - zl).astype(BF16), "zl", FLIP)
    far, fill = lax.optimization_barrier((far, fill))
    return half(v, zl) + far.astype(F32), fill


def sum_group(v):
    v = v + lax.ppermute(v, "c", FLIP)
    return v + lax.ppermute(v, "zl", FLIP)


def gather_weight(w, axis):
    moved = lax.ppermute(w, ("c", "zh"), MOVE)
    swapped = swap(w)
    pair = ordered(swapped, moved, lax.axis_index("zh"), axis)
    return lax.all_gather(pair, "p", axis=axis, tiled=True)


def scatter_chips(g):
    part = lax.psum_scatter(g, "p", scatter_dimension=0, tiled=True)
    return part.reshape(2, -1, part.shape[1])


def group_norm(values):
    mean, scale = moments(values)
    return (values - mean) * scale


def gelu_tanh(values):
    return jax.nn.gelu(values, approximate=True)


def gated(gate_pre, grouped):
    return jax.nn.silu(gate_pre) * grouped


def decay_weights(running):
    span = running.shape[1]
    gap = running[:, :, None] - running[:, None, :]
    lower = jnp.arange(span)[:, None] >= jnp.arange(span)[None, :]
    return jnp.where(lower[None], jnp.exp(jnp.minimum(gap, 0.0)), 0.0)


def dot(a, b, dims):
    return lax.dot_general(a, b, (dims, ((), ())), preferred_element_type=F32)


def norm_back(d, low, mean, scale, gain, width):
    hat = (low.astype(F32) - mean) * scale
    scaled = d * gain
    sums = sum_group(jnp.stack([jnp.sum(scaled, 1), jnp.sum(scaled * hat, 1)])) / width
    d_in = scale * (scaled - sums[0][:, None] - hat * sums[1][:, None])
    return d_in, jnp.sum(d * hat, 0)


def on_device(
    tokens,
    gain_attn,
    gain_ffn,
    w_query,
    w_key,
    w_value,
    w_gate,
    w_out,
    w_up,
    w_down,
    log_decay,
    cotangent,
):
    rows = tokens.shape[0]
    heads = log_decay.shape[0]
    cols = tokens.shape[1]
    block = 2 * lax.axis_index("p") + lax.axis_index("zh")
    blocks = 2 * lax.axis_size("p")

    extra = jnp.stack([gain_attn, gain_ffn])
    tokens = jnp.concatenate([tokens, jnp.pad(extra, ((0, 14), (0, 0)))])
    decay = jnp.pad(log_decay, ((0, 8 - heads), (0, 0)))
    gathered = gather_and_project(
        blocks // 2, decay, w_query, w_key, w_value, w_gate, w_out.T, tokens, cotangent
    )
    full_decay, full_query, full_key, full_value, full_gate, full_out = gathered[:6]
    grad_full, tokens_own, grad_own, gains, normed, query_rows = gathered[6:12]
    key_rows, value_rows, gate_pre, stats = gathered[12:]
    full_query, full_key, full_value, full_gate, full_out = (
        f.reshape(-1, f.shape[2]) for f in (full_query, full_key, full_value, full_gate, full_out)
    )
    full_up = gather_weight(w_up, 0)
    full_down = gather_weight(w_down.T, 0)
    width = normed.shape[1]
    key_width = full_query.shape[1] // heads
    value_width = full_value.shape[1] // heads
    gain_two = gains[1].astype(F32)
    gain_one_own, gain_two_own = tokens_own[rows].astype(F32), tokens_own[rows + 1].astype(F32)
    tokens_own = tokens_own[:rows]
    mean_one, scale_one = stats[0, :, :1], stats[1, :, :1]
    block_sums = jnp.sum(full_decay[:, :heads], axis=2)
    log_decay = lax.dynamic_index_in_dim(full_decay, block, 0, False)[:heads]

    nn = ((1,), (0,))
    nt = ((1,), (1,))
    tn = ((0,), (0,))
    query_rows = query_rows.reshape(rows, heads, key_width)
    key_rows = key_rows.reshape(rows, heads, key_width)
    value_rows = value_rows.reshape(rows, heads, value_width)
    running = jnp.cumsum(log_decay, axis=1)
    block_decay = running[:, -1]
    query_scale = jnp.exp(running).T[:, :, None]
    key_scale = jnp.exp(block_decay[:, None] - running).T[:, :, None]
    key_decay = (key_rows * key_scale).astype(BF16)
    query_decay = (query_rows * query_scale).astype(BF16)

    def einsum(spec, a, b):
        return jnp.einsum(spec, a, b, preferred_element_type=F32)

    place = jnp.arange(blocks)[:, None]

    def decay_over(first, last):
        inside = (place >= first) & (place < last)
        return jnp.exp(jnp.sum(jnp.where(inside, block_sums, 0.0), axis=0))[:, None, None]

    def exchanged(v, stride):
        if stride == 1:
            return lax.ppermute(v, "zh", FLIP)
        pairs = [(i, i ^ (stride // 2)) for i in range(blocks // 2)]
        return lax.ppermute(v, "p", pairs)

    def carried(part, backward, fill=()):
        total, carry = part, jnp.zeros_like(part)
        stride = 1
        while stride < blocks:
            middle = block // (2 * stride) * (2 * stride) + stride
            high = block >= middle
            low_decay = decay_over(middle - stride, middle)
            high_decay = decay_over(middle, middle + stride)
            other, fill = lax.optimization_barrier((exchanged(total.astype(BF16), stride), fill))
            other = other.astype(F32)
            if backward:
                carry = jnp.where(high, carry, carry + decay_over(block + 1, middle) * other)
                total = jnp.where(high, other + low_decay * total, total + low_decay * other)
            else:
                carry = jnp.where(high, carry + decay_over(middle, block) * other, carry)
                total = jnp.where(high, high_decay * other + total, high_decay * total + other)
            stride *= 2
        return carry.astype(BF16), fill

    state, _ = carried(einsum("nhd,nhe->hde", key_decay, value_rows), False)
    decays = decay_weights(running)
    weighted = (einsum("nhd,mhd->hnm", query_rows, key_rows) * decays).astype(BF16)
    retained = einsum("hnm,mhe->nhe", weighted, value_rows) + einsum(
        "nhd,hde->nhe", query_decay, state
    )
    grouped = group_norm(retained).reshape(rows, heads * value_width)
    mixed_rows = gated(gate_pre, grouped).astype(BF16)
    attended, _ = scatter_group(dot(mixed_rows, full_out, nt))
    hidden = tokens_own.astype(F32) + attended
    hidden_own = hidden.astype(BF16)
    hidden_full, d_act = gather_group(hidden_own, dot(grad_full, full_down, nn))
    hidden_full = hidden_full.astype(F32)
    mean_two, scale_two = moments(hidden_full)
    normed_ffn = ((hidden_full - mean_two) * scale_two * gain_two).astype(BF16)
    pre_act = dot(normed_ffn, full_up, nn)
    activated, gelu_back = jax.vjp(gelu_tanh, pre_act)
    activated = activated.astype(BF16)
    d_pre = gelu_back(d_act)[0].astype(BF16)
    d_normed_ffn, grad_down = scatter_group(
        dot(d_pre, full_up, nt), dot(grad_full, activated, tn).astype(BF16)
    )
    part_down = scatter_chips(grad_down)
    ffn, _ = scatter_group(dot(activated, full_down, nt))
    output = (hidden + ffn).astype(BF16)
    d_hidden_norm, d_gain_two = norm_back(
        d_normed_ffn, hidden_own, mean_two, scale_two, gain_two_own, width
    )
    d_hidden = grad_own.astype(F32) + d_hidden_norm
    d_attended, grad_up = gather_group(
        d_hidden.astype(BF16), dot(normed_ffn, d_pre, tn).astype(BF16)
    )
    part_up = scatter_chips(grad_up)
    d_mixed = dot(d_attended, full_out, nn)
    _, gate_back = jax.vjp(gated, gate_pre, grouped)
    d_gate, d_grouped = gate_back(d_mixed)
    d_gate = d_gate.astype(BF16)
    _, group_back = jax.vjp(group_norm, retained)
    d_retained = group_back(d_grouped.reshape(rows, heads, value_width))[0].astype(BF16)
    later_grad, grad_out = carried(
        einsum("nhd,nhe->hde", query_decay, d_retained),
        True,
        dot(d_attended, mixed_rows, tn).astype(BF16),
    )
    part_out = scatter_chips(grad_out)
    d_raw = (einsum("nhe,mhe->hnm", d_retained, value_rows) * decays).astype(BF16)
    d_query = (
        einsum("hnm,mhd->nhd", d_raw, key_rows)
        + einsum("nhe,hde->nhd", d_retained, state) * query_scale
    )
    d_query = d_query.astype(BF16).reshape(rows, heads * key_width)
    d_keys = (
        einsum("hnm,nhd->mhd", d_raw, query_rows)
        + einsum("mhe,hde->mhd", value_rows, later_grad) * key_scale
    )
    d_keys = d_keys.astype(BF16).reshape(rows, heads * key_width)
    d_values = einsum("hnm,nhe->mhe", weighted, d_retained) + einsum(
        "mhd,hde->mhe", key_decay, later_grad
    )
    d_values = d_values.astype(BF16).reshape(rows, heads * value_width)
    turned = normed.T
    d_normed, first = scatter_group(
        dot(d_gate, full_gate, nt)
        + dot(d_query, full_query, nt)
        + dot(d_keys, full_key, nt)
        + dot(d_values, full_value, nt),
        reduce_gradients(blocks // 2, 1, turned, (d_gate, d_values)),
    )
    grad_gate, grad_value = first
    d_tokens_norm, d_gain_one = norm_back(
        d_normed, tokens_own, mean_one, scale_one, gain_one_own, width
    )
    input_grad = (d_hidden + d_tokens_norm).astype(BF16)
    gain = jnp.concatenate([d_gain_one[None], d_gain_two[None], jnp.zeros((6, cols), F32)])
    grad_query, grad_key, grad_down, grad_up, grad_out, output, input_grad, gain = reduce_gradients(
        blocks // 2,
        2,
        turned,
        (d_query, d_keys),
        (part_down, part_up, part_out),
        (output, input_grad),
        (gain,),
    )
    return (
        output,
        input_grad.astype(F32),
        gain[0],
        gain[1],
        grad_query,
        grad_key,
        grad_value,
        grad_gate,
        grad_out.T,
        grad_up,
        grad_down.T,
    )


def solution(mesh):
    seq, head = mesh.devices.shape
    finer = Mesh(mesh.devices.reshape(seq // 2, 2, head // 2, 2), ("p", "c", "zh", "zl"))
    seq, head = ("p", "c"), ("zh", "zl")
    by_row, by_column, one = P(seq, head), P(head, seq), P(head)
    in_specs = (
        (by_row, one, one) + (by_row,) * 4 + (by_column, by_row, by_column) + (by_column, by_row)
    )
    out_specs = (by_row, by_row, one, one) + (by_row,) * 4 + (by_column, by_row, by_column)
    return jax.shard_map(
        on_device, mesh=finer, in_specs=in_specs, out_specs=out_specs, check_vma=False
    )
```

```python
import functools

import jax
import jax.numpy as jnp
from jax import lax
from jax.experimental import pallas as pl
from jax.experimental.pallas import tpu as pltpu
from jax.sharding import Mesh
from jax.sharding import PartitionSpec as P

F32 = jnp.float32
BF16 = jnp.bfloat16

SWAP = ((0, 0), (1, 2), (2, 1), (3, 3))
MOVE = ((0, 1), (1, 3), (2, 0), (3, 2))
BACK = ((1, 0), (3, 1), (0, 2), (2, 3))
FLIP = ((0, 1), (1, 0))


def moments(values):
    mean = jnp.mean(values, axis=-1, keepdims=True)
    centered = values - mean
    spread = jnp.mean(centered * centered, axis=-1, keepdims=True)
    return mean, lax.rsqrt(spread + 1e-05)


MESH = pl.DeviceIdType.MESH


def bits_of(count):
    return count.bit_length() - 1


def flipped(index, stride):
    return index + stride * (1 - 2 * lax.rem(lax.div(index, stride), 2))


class Place:
    def __init__(self, chips):
        self.p, self.c = lax.axis_index("p"), lax.axis_index("c")
        self.zh, self.zl = lax.axis_index("zh"), lax.axis_index("zl")
        self.bits = bits_of(chips)
        self.crossed = lax.rem(self.c + self.zh, 2)
        self.core = {"c": 1 - self.c}
        self.high = {"zh": 1 - self.zh}
        self.diagonal = {"c": 1 - self.c, "zh": 1 - self.zh}
        self.low = {"zl": 1 - self.zl}

    def chip(self, bit):
        return {"p": flipped(self.p, 2**bit)}

    def meet(self):
        barrier = pltpu.get_barrier_semaphore()
        partners = [self.core, self.high, self.diagonal, self.low]
        partners += [self.chip(bit) for bit in range(self.bits)]
        for partner in partners:
            pl.semaphore_signal(barrier, inc=1, device_id=partner, device_id_type=MESH)
        pl.semaphore_wait(barrier, len(partners))

    def moved_to(self):
        return {
            "c": self.c + self.crossed * (1 - 2 * self.c),
            "zh": self.zh + (1 - self.crossed) * (1 - 2 * self.zh),
        }


def remote(src, dst, send, recv, device):
    return pltpu.make_async_remote_copy(
        src_ref=src,
        dst_ref=dst,
        send_sem=send,
        recv_sem=recv,
        device_id=device,
        device_id_type=MESH,
    )


class Relabel:
    def __init__(self, place, src, dst, send, recv):
        self.place = place
        self.moved = remote(src, dst, send.at[0], recv.at[0], place.moved_to())
        self.swapped = remote(src, dst, send.at[1], recv.at[1], place.diagonal)
        self.kept = pltpu.make_async_copy(src, dst, recv.at[1])

    def start(self):
        self.moved.start()
        pl.when(self.place.crossed == 1)(self.swapped.start)
        pl.when(self.place.crossed == 0)(self.kept.start)

    def arrive(self):
        self.moved.wait_recv()
        pl.when(self.place.crossed == 1)(self.swapped.wait_recv)
        pl.when(self.place.crossed == 0)(self.kept.wait)

    def finish(self):
        self.moved.wait_send()
        pl.when(self.place.crossed == 1)(self.swapped.wait_send)


class Spread:
    def __init__(self, place, dst, send, recv):
        self.place, self.dst, self.send, self.recv = place, dst, send, recv
        self.orders = [list(range(place.bits)), list(reversed(range(place.bits)))]

    def copy(self, h, step, mask):
        order = self.orders[h]
        block = self.place.p
        for at in range(self.place.bits):
            if mask >> at & 1:
                block = flipped(block, 2 ** order[at])
        ref = self.dst.at[2 * block + h]
        name = mask + 2**step
        return remote(ref, ref, self.send.at[h, name], self.recv.at[h, name], self.place.chip(order[step]))

    def start(self):
        for step in range(self.place.bits):
            for h in range(2):
                self.copy(h, step, 0).start()

    def arrive(self, mask):
        for h in range(2):
            top = bits_of(mask)
            self.copy(h, top, mask - 2**top).wait_recv()
            for step in range(top + 1, self.place.bits):
                self.copy(h, step, mask).start()

    def rest(self, since):
        for mask in range(since, 2**self.place.bits):
            self.arrive(mask)

    def finish(self):
        for h in range(2):
            for mask in range(1, 2**self.place.bits):
                top = bits_of(mask)
                self.copy(h, top, mask - 2**top).wait_send()


class Columns:
    def __init__(self, place, src, full, send, recv):
        self.place = place
        cols = src.shape[1]

        def at(zl, c):
            return full.at[:, pl.ds(pl.multiple_of((2 * c + zl) * cols, cols), cols)]

        own, near = at(place.zl, place.c), at(1 - place.zl, place.c)
        self.own = own
        crossing = at(place.zl, 1 - place.c)
        self.swapped = remote(src, crossing, send.at[0], recv.at[0], place.diagonal)
        self.kept = pltpu.make_async_copy(src, own, recv.at[0])
        self.low = remote(own, own, send.at[1], recv.at[1], place.low)
        self.core = remote(own, own, send.at[2], recv.at[2], place.core)
        self.passed = remote(near, near, send.at[3], recv.at[3], place.core)

    def start(self):
        pl.when(self.place.crossed == 1)(self.swapped.start)
        pl.when(self.place.crossed == 0)(self.kept.start)

    def second(self):
        pl.when(self.place.crossed == 1)(self.swapped.wait_recv)
        pl.when(self.place.crossed == 0)(self.kept.wait)
        self.low.start()
        self.core.start()

    def third(self):
        self.low.wait_recv()
        self.passed.start()

    def finish(self):
        pl.when(self.place.crossed == 1)(self.swapped.wait_send)
        self.low.wait_send()
        self.core.wait_send()
        self.passed.wait_send()


def project_kernel(chips, *refs):
    decay, query, key, value, gate, out, tokens, cotangent = refs[:8]
    results = refs[8:23]
    full_decay, full_query, full_key, full_value, full_gate, full_out = results[:6]
    grad_full, tokens_own, gains, normed, query_rows = results[6:11]
    key_rows, value_rows, gate_pre, stats = results[11:]
    every, weight, zsend, zrecv, send, recv, tsend, trecv, local = refs[23:]
    place = Place(chips)
    place.meet()
    shards = [decay, query, key, value, gate, out]
    fulls = [full_decay, full_query, full_key, full_value, full_gate, full_out]
    slots = [f.at[2 * place.p + place.c] for f in fulls[:5]] + [full_out.at[place.c]]
    labels = [Relabel(place, s, t, zsend.at[i], zrecv.at[i]) for i, (s, t) in enumerate(zip(shards, slots))]
    spreads = [Spread(place, f, send.at[i], recv.at[i]) for i, f in enumerate(fulls[:5])]
    held = Columns(place, tokens, every, tsend.at[0], trecv.at[0])
    grads = Columns(place, cotangent, grad_full, tsend.at[1], trecv.at[1])
    for i in range(4):
        labels[i].start()
    held.start()

    def spread(i):
        labels[i].arrive()
        spreads[i].start()

    count = tokens.shape[0] - 16
    tile = min(128, count)

    def norm():
        gain = every[count : count + 1, :].astype(F32)

        def one(i, carry):
            at = pl.ds(pl.multiple_of(i * tile, tile), tile)
            v = every[at, :].astype(F32)
            mean, scale = moments(v)
            normed[at, :] = ((v - mean) * scale * gain).astype(BF16)
            stats[0, at, :] = jnp.broadcast_to(mean, (tile, 128))
            stats[1, at, :] = jnp.broadcast_to(scale, (tile, 128))
            return carry

        lax.fori_loop(0, count // tile, one, 0)

    step = min(256, count)

    def project(i, rows):
        spreads[i].rest(2)
        full = fulls[i]
        slots, height, columns = full.shape
        held_weight = weight.at[:, :, pl.ds(0, columns)]
        copy = pltpu.make_async_copy(full, held_weight, local.at[0])
        copy.start()
        copy.wait()

        def one(j, carry):
            at = pl.ds(pl.multiple_of(j * step, step), step)
            w = held_weight[...].reshape(slots * height, columns)
            v = jnp.dot(normed[at, :], w, preferred_element_type=F32)
            rows[at, :] = v.astype(rows.dtype)
            return carry

        lax.fori_loop(0, count // step, one, 0)

    spread(0)
    spread(1)
    spread(2)
    spreads[0].arrive(1)
    spreads[1].arrive(1)
    spread(3)
    spreads[2].arrive(1)
    held.second()
    held.core.wait_recv()
    labels[4].start()
    labels[5].start()
    grads.start()
    spreads[3].arrive(1)
    held.third()
    spread(4)
    held.passed.wait_recv()
    norm()
    project(1, query_rows)
    project(2, key_rows)
    labels[5].arrive()
    spreads[4].arrive(1)
    project(3, value_rows)
    grads.second()
    project(4, gate_pre)
    grads.third()
    spreads[0].rest(2)
    grads.core.wait_recv()
    grads.passed.wait_recv()
    keep = [
        pltpu.make_async_copy(held.own, tokens_own, local.at[1]),
        pltpu.make_async_copy(every.at[pl.ds(count, 16)], gains, local.at[2]),
    ]
    for copy in keep:
        copy.start()
    for label in labels:
        label.finish()
    for each in spreads:
        each.finish()
    held.finish()
    grads.finish()
    for copy in keep:
        copy.wait()


def gather_and_project(chips, decay, query, key, value, gate, out, tokens, cotangent):
    shards = [decay, query, key, value, gate, out]
    rows, cols = tokens.shape[0] - 16, tokens.shape[1]
    width = 4 * cols
    slots = 2 * chips
    shape = jax.ShapeDtypeStruct
    vmem = pl.BlockSpec(memory_space=pltpu.VMEM)
    hbm = pl.BlockSpec(memory_space=pl.ANY)
    gathered = [shape((slots, *s.shape), s.dtype) for s in shards[:5]]
    gathered.append(shape((2, *out.shape), out.dtype))
    wide = [query.shape[1], key.shape[1], value.shape[1], gate.shape[1]]
    made = [
        shape((rows, width), BF16),
        shape((tokens.shape[0], cols), BF16),
        shape((16, width), BF16),
        shape((rows, width), BF16),
        shape((rows, wide[0]), BF16),
        shape((rows, wide[1]), BF16),
        shape((rows, wide[2]), BF16),
        shape((rows, wide[3]), F32),
        shape((2, rows, 128), F32),
    ]
    names = 2 ** bits_of(chips)
    dma = pltpu.SemaphoreType.DMA
    flops = 2 * rows * width * sum(wide)
    return pl.pallas_call(
        functools.partial(project_kernel, chips),
        out_shape=gathered + made,
        in_specs=[vmem] * 8,
        out_specs=[hbm] * 9 + [vmem] * 6,
        scratch_shapes=[
            pltpu.VMEM((tokens.shape[0], width), BF16),
            pltpu.VMEM((slots, value.shape[0], value.shape[1]), BF16),
            dma((6, 2)),
            dma((6, 2)),
            dma((5, 2, names)),
            dma((5, 2, names)),
            dma((2, 4)),
            dma((2, 4)),
            dma((3,)),
        ],
        compiler_params=pltpu.CompilerParams(
            collective_id=0, has_side_effects=True, vmem_limit_bytes=60 * 2**20
        ),
        cost_estimate=pl.CostEstimate(flops=flops, bytes_accessed=60 * 2**20, transcendentals=0),
        name="gather_project",
    )(*shards, tokens, cotangent)


def reduce_kernel(chips, count, ready_count, swap_count, gains, *refs):
    refs = list(refs)

    def taken(number):
        front = refs[:number]
        del refs[:number]
        return front

    (turned,) = taken(1)
    grads, ready, swaps, gain = taken(count), taken(ready_count), taken(swap_count), taken(gains)
    results, totals, swapped_to = taken(count), taken(ready_count), taken(swap_count)
    gain_to = taken(gains)
    parts, arrived, handed = taken(count), taken(count), taken(count)
    ready_handed = taken(ready_count)
    send, recv, zsend, zrecv = taken(4)
    place = Place(chips)
    place.meet()
    bits = place.bits
    orders = [list(range(bits)), list(reversed(range(bits)))]
    back = {
        "c": place.c + (1 - place.crossed) * (1 - 2 * place.c),
        "zh": place.zh + place.crossed * (1 - 2 * place.zh),
    }

    def slot(h, mask):
        block = place.p
        for at in range(bits):
            if mask >> at & 1:
                block = flipped(block, 2 ** orders[h][at])
        return 2 * block + h

    def added(target, first, second):
        height = first.shape[0]
        step = min(64, height)

        def one(i, carry):
            at = pl.ds(pl.multiple_of(i * step, step), step)
            v = first[at, :].astype(F32) + second[at, :].astype(F32)
            target[at, :] = v.astype(target.dtype)
            return carry

        lax.fori_loop(0, height // step, one, 0)

    def hop(i, h, step, mask):
        name = mask + 2**step
        return remote(
            parts[i].at[slot(h, name)],
            arrived[i].at[h, name],
            send.at[i, h, name],
            recv.at[i, h, name],
            place.chip(orders[h][step]),
        )

    def give(i, step):
        for mask in reversed(range(2**step)):
            for h in range(2):
                hop(i, h, step, mask).start()

    def take(i, step):
        for mask in reversed(range(2**step)):
            for h in range(2):
                hop(i, h, step, mask).wait_recv()
                mine = parts[i].at[slot(h, mask)]
                added(mine, mine, arrived[i].at[h, 2**step + mask])

    def hand(i):
        if i < count:
            even, odd, to = parts[i].at[2 * place.p + 1 - place.zh], own(i), handed[i]
        else:
            even, odd, to = ready[i - count].at[1 - place.zh], own(i), ready_handed[i - count]
        moved = remote(even, to.at[0], zsend.at[i, 0], zrecv.at[i, 0], back)
        swapped = remote(odd, to.at[1], zsend.at[i, 1], zrecv.at[i, 1], place.diagonal)
        return moved, swapped

    def own(i):
        if i < count:
            return parts[i].at[2 * place.p + place.zh]
        return ready[i - count].at[place.zh]

    def hand_out(i):
        moved, swapped = hand(i)
        moved.start()
        pl.when(place.crossed == 1)(swapped.start)

    def settle(i):
        to = handed[i] if i < count else ready_handed[i - count]
        result = results[i] if i < count else totals[i - count]
        moved, swapped = hand(i)
        moved.wait_recv()

        @pl.when(place.crossed == 1)
        def _():
            swapped.wait_recv()
            added(result, to.at[0], to.at[1])

        @pl.when(place.crossed == 0)
        def _():
            added(result, to.at[0], own(i))

    def swapping(i):
        src, dst = swaps[i], swapped_to[i]
        at = count + ready_count + i
        over = remote(src, dst, zsend.at[at, 0], zrecv.at[at, 0], place.diagonal)
        return over, pltpu.make_async_copy(src, dst, zrecv.at[at, 0])

    def multiply(i):
        slots, height, _ = parts[i].shape

        def one(s, carry):
            at = pl.ds(pl.multiple_of(s * height, height), height)
            v = jnp.dot(turned[at, :], grads[i][...], preferred_element_type=F32)
            parts[i][s] = v.astype(BF16)
            return carry

        lax.fori_loop(0, slots, one, 0)

    def stage(i, at):
        if at == 0:
            multiply(i)
            give(i, bits - 1)
        elif at < bits:
            take(i, bits - at)
            give(i, bits - at - 1)
        elif at == bits:
            take(i, 0)
            hand_out(i)
        else:
            settle(i)

    for i in range(ready_count):
        hand_out(count + i)
    for i in range(swap_count):
        over, kept = swapping(i)
        pl.when(place.crossed == 1)(over.start)
        pl.when(place.crossed == 0)(kept.start)
    if gains:
        steps, landed, gsend, grecv = taken(4)
        partners = [place.high] + [place.chip(bit) for bit in range(bits)]

        def step(k):
            return remote(steps.at[k], landed.at[k], gsend.at[k], grecv.at[k], partners[k])

        over = remote(steps.at[bits + 1], gain_to[0], gsend.at[bits + 1], grecv.at[bits + 1], place.diagonal)
        kept = pltpu.make_async_copy(steps.at[bits + 1], gain_to[0], grecv.at[bits + 1])
        steps[0] = gain[0][...]
        step(0).start()
    for tick in range(count + bits + 1):
        for at in range(bits + 2):
            if 0 <= tick - at < count:
                stage(tick - at, at)
    if gains:
        for k in range(bits + 1):
            step(k).wait_recv()
            steps[k + 1] = steps[k] + landed[k]
            if k < bits:
                step(k + 1).start()
        pl.when(place.crossed == 1)(over.start)
        pl.when(place.crossed == 0)(kept.start)
    for i in range(ready_count):
        settle(count + i)
    for i in range(count):
        for h in range(2):
            for at in range(bits):
                for mask in range(2**at):
                    hop(i, h, at, mask).wait_send()
    for i in range(count + ready_count):
        moved, swapped = hand(i)
        moved.wait_send()
        pl.when(place.crossed == 1)(swapped.wait_send)
    if gains:
        for k in range(bits + 1):
            step(k).wait_send()
        pl.when(place.crossed == 1)(over.wait)
        pl.when(place.crossed == 0)(kept.wait)
    for i in range(swap_count):
        over, kept = swapping(i)
        pl.when(place.crossed == 1)(over.wait)
        pl.when(place.crossed == 0)(kept.wait)


def reduce_gradients(chips, identity, turned, grads, ready=(), swaps=(), gain=()):
    count = len(grads)
    width, rows = turned.shape
    slots = 2 * chips
    height = width // slots
    vmem = pl.BlockSpec(memory_space=pltpu.VMEM)
    wide = [g.shape[1] for g in grads]
    shape = jax.ShapeDtypeStruct
    dma = pltpu.SemaphoreType.DMA
    moves = count + len(ready) + len(swaps)
    hops = bits_of(chips) + 2
    extra = []
    if gain:
        extra = [pltpu.VMEM((hops, *gain[0].shape), F32)] * 2 + [dma((hops,)), dma((hops,))]
    results = pl.pallas_call(
        functools.partial(reduce_kernel, chips, count, len(ready), len(swaps), len(gain)),
        out_shape=[shape((height, w), F32) for w in wide]
        + [shape(r.shape[1:], F32) for r in ready]
        + [shape(v.shape, v.dtype) for v in (*swaps, *gain)],
        in_specs=[vmem] * (1 + moves + len(gain)),
        out_specs=[vmem] * (moves + len(gain)),
        scratch_shapes=[pltpu.VMEM((slots, height, w), BF16) for w in wide]
        + [pltpu.VMEM((2, chips, height, w), BF16) for w in wide]
        + [pltpu.VMEM((2, height, w), BF16) for w in wide]
        + [pltpu.VMEM(r.shape, BF16) for r in ready]
        + [dma((count, 2, chips)), dma((count, 2, chips)), dma((moves, 2)), dma((moves, 2))]
        + extra,
        compiler_params=pltpu.CompilerParams(
            collective_id=identity, has_side_effects=True, vmem_limit_bytes=60 * 2**20
        ),
        cost_estimate=pl.CostEstimate(
            flops=2 * rows * width * sum(wide), bytes_accessed=60 * 2**20, transcendentals=0
        ),
        name=f"reduce_gradients_{identity}",
    )(turned, *grads, *ready, *swaps, *gain)
    return results


def swap(v):
    return lax.ppermute(v, ("c", "zh"), SWAP)


def ordered(first, second, flag, axis):
    return jnp.where(
        flag == 0,
        jnp.concatenate([first, second], axis),
        jnp.concatenate([second, first], axis),
    )


def gather_group(v, fill=()):
    far, fill = lax.optimization_barrier((lax.ppermute(v, "zl", FLIP), fill))
    near = ordered(v, far, lax.axis_index("zl"), 1)
    return ordered(near, lax.ppermute(near, "c", FLIP), lax.axis_index("c"), 1), fill


def half(v, which):
    size = v.shape[1] // 2
    return lax.dynamic_slice_in_dim(v, which * size, size, 1)


def scatter_group(v, fill=()):
    c, zl = lax.axis_index("c"), lax.axis_index("zl")
    far = lax.ppermute(half(v, 1 - c).astype(BF16), "c", FLIP)
    v = half(v, c) + far.astype(F32)
    far = lax.ppermute(half(v, 1 - zl).astype(BF16), "zl", FLIP)
    far, fill = lax.optimization_barrier((far, fill))
    return half(v, zl) + far.astype(F32), fill


def sum_group(v):
    v = v + lax.ppermute(v, "c", FLIP)
    return v + lax.ppermute(v, "zl", FLIP)


def gather_weight(w, axis):
    moved = lax.ppermute(w, ("c", "zh"), MOVE)
    swapped = swap(w)
    pair = ordered(swapped, moved, lax.axis_index("zh"), axis)
    return lax.all_gather(pair, "p", axis=axis, tiled=True)


def scatter_chips(g):
    part = lax.psum_scatter(g, "p", scatter_dimension=0, tiled=True)
    return part.reshape(2, -1, part.shape[1])


def group_norm(values):
    mean, scale = moments(values)
    return (values - mean) * scale


def gelu_tanh(values):
    return jax.nn.gelu(values, approximate=True)


def gated(gate_pre, grouped):
    return jax.nn.silu(gate_pre) * grouped


def decay_weights(running):
    span = running.shape[1]
    gap = running[:, :, None] - running[:, None, :]
    lower = jnp.arange(span)[:, None] >= jnp.arange(span)[None, :]
    return jnp.where(lower[None], jnp.exp(jnp.minimum(gap, 0.0)), 0.0)


def dot(a, b, dims):
    return lax.dot_general(a, b, (dims, ((), ())), preferred_element_type=F32)


def norm_back(d, low, mean, scale, gain, width):
    hat = (low.astype(F32) - mean) * scale
    scaled = d * gain
    sums = sum_group(jnp.stack([jnp.sum(scaled, 1), jnp.sum(scaled * hat, 1)])) / width
    d_in = scale * (scaled - sums[0][:, None] - hat * sums[1][:, None])
    return d_in, jnp.sum(d * hat, 0)


def on_device(
    tokens,
    gain_attn,
    gain_ffn,
    w_query,
    w_key,
    w_value,
    w_gate,
    w_out,
    w_up,
    w_down,
    log_decay,
    cotangent,
):
    rows = tokens.shape[0]
    heads = log_decay.shape[0]
    cols = tokens.shape[1]
    block = 2 * lax.axis_index("p") + lax.axis_index("zh")
    blocks = 2 * lax.axis_size("p")

    extra = jnp.stack([gain_attn, gain_ffn])
    tokens = jnp.concatenate([tokens, jnp.pad(extra, ((0, 14), (0, 0)))])
    decay = jnp.pad(log_decay, ((0, 8 - heads), (0, 0)))
    gathered = gather_and_project(
        blocks // 2, decay, w_query, w_key, w_value, w_gate, w_out.T, tokens, cotangent
    )
    full_decay, full_query, full_key, full_value, full_gate, full_out = gathered[:6]
    grad_full, tokens_own, gains, normed, query_rows = gathered[6:11]
    key_rows, value_rows, gate_pre, stats = gathered[11:]
    quarter = 2 * lax.axis_index("c") + lax.axis_index("zl")
    grad_own = lax.dynamic_slice_in_dim(grad_full, quarter * cols, cols, 1)
    full_query, full_key, full_value, full_gate, full_out = (
        f.reshape(-1, f.shape[2]) for f in (full_query, full_key, full_value, full_gate, full_out)
    )
    full_out = lax.all_gather(full_out, "p", axis=0, tiled=True)
    full_up = gather_weight(w_up, 0)
    full_down = gather_weight(w_down.T, 0)
    width = normed.shape[1]
    key_width = full_query.shape[1] // heads
    value_width = full_value.shape[1] // heads
    gain_two = gains[1].astype(F32)
    gain_one_own, gain_two_own = tokens_own[rows].astype(F32), tokens_own[rows + 1].astype(F32)
    tokens_own = tokens_own[:rows]
    mean_one, scale_one = stats[0, :, :1], stats[1, :, :1]
    block_sums = jnp.sum(full_decay[:, :heads], axis=2)
    log_decay = lax.dynamic_index_in_dim(full_decay, block, 0, False)[:heads]

    nn = ((1,), (0,))
    nt = ((1,), (1,))
    tn = ((0,), (0,))
    query_rows = query_rows.reshape(rows, heads, key_width)
    key_rows = key_rows.reshape(rows, heads, key_width)
    value_rows = value_rows.reshape(rows, heads, value_width)
    running = jnp.cumsum(log_decay, axis=1)
    block_decay = running[:, -1]
    query_scale = jnp.exp(running).T[:, :, None]
    key_scale = jnp.exp(block_decay[:, None] - running).T[:, :, None]
    key_decay = (key_rows * key_scale).astype(BF16)
    query_decay = (query_rows * query_scale).astype(BF16)

    def einsum(spec, a, b):
        return jnp.einsum(spec, a, b, preferred_element_type=F32)

    place = jnp.arange(blocks)[:, None]

    def decay_over(first, last):
        inside = (place >= first) & (place < last)
        return jnp.exp(jnp.sum(jnp.where(inside, block_sums, 0.0), axis=0))[:, None, None]

    def exchanged(v, stride):
        if stride == 1:
            return lax.ppermute(v, "zh", FLIP)
        pairs = [(i, i ^ (stride // 2)) for i in range(blocks // 2)]
        return lax.ppermute(v, "p", pairs)

    def carried(part, backward, fill=()):
        total, carry = part, jnp.zeros_like(part)
        stride = 1
        while stride < blocks:
            middle = block // (2 * stride) * (2 * stride) + stride
            high = block >= middle
            low_decay = decay_over(middle - stride, middle)
            high_decay = decay_over(middle, middle + stride)
            other, fill = lax.optimization_barrier((exchanged(total.astype(BF16), stride), fill))
            other = other.astype(F32)
            if backward:
                carry = jnp.where(high, carry, carry + decay_over(block + 1, middle) * other)
                total = jnp.where(high, other + low_decay * total, total + low_decay * other)
            else:
                carry = jnp.where(high, carry + decay_over(middle, block) * other, carry)
                total = jnp.where(high, high_decay * other + total, high_decay * total + other)
            stride *= 2
        return carry.astype(BF16), fill

    state, _ = carried(einsum("nhd,nhe->hde", key_decay, value_rows), False)
    decays = decay_weights(running)
    weighted = (einsum("nhd,mhd->hnm", query_rows, key_rows) * decays).astype(BF16)
    retained = einsum("hnm,mhe->nhe", weighted, value_rows) + einsum(
        "nhd,hde->nhe", query_decay, state
    )
    grouped = group_norm(retained).reshape(rows, heads * value_width)
    mixed_rows = gated(gate_pre, grouped).astype(BF16)
    attended, turned = scatter_group(dot(mixed_rows, full_out, nt), normed.T)
    hidden = tokens_own.astype(F32) + attended
    hidden_own = hidden.astype(BF16)
    hidden_full, d_act = gather_group(hidden_own, dot(grad_full, full_down, nn))
    hidden_full = hidden_full.astype(F32)
    mean_two, scale_two = moments(hidden_full)
    normed_ffn = ((hidden_full - mean_two) * scale_two * gain_two).astype(BF16)
    pre_act = dot(normed_ffn, full_up, nn)
    activated, gelu_back = jax.vjp(gelu_tanh, pre_act)
    activated = activated.astype(BF16)
    d_pre = gelu_back(d_act)[0].astype(BF16)
    d_normed_ffn, grad_down = scatter_group(
        dot(d_pre, full_up, nt), dot(grad_full, activated, tn).astype(BF16)
    )
    part_down = scatter_chips(grad_down)
    ffn, _ = scatter_group(dot(activated, full_down, nt))
    output = (hidden + ffn).astype(BF16)
    d_hidden_norm, d_gain_two = norm_back(
        d_normed_ffn, hidden_own, mean_two, scale_two, gain_two_own, width
    )
    d_hidden = grad_own.astype(F32) + d_hidden_norm
    d_attended, grad_up = gather_group(
        d_hidden.astype(BF16), dot(normed_ffn, d_pre, tn).astype(BF16)
    )
    part_up = scatter_chips(grad_up)
    d_mixed = dot(d_attended, full_out, nn)
    _, gate_back = jax.vjp(gated, gate_pre, grouped)
    d_gate, d_grouped = gate_back(d_mixed)
    d_gate = d_gate.astype(BF16)
    _, group_back = jax.vjp(group_norm, retained)
    d_retained = group_back(d_grouped.reshape(rows, heads, value_width))[0].astype(BF16)
    later_grad, grad_out = carried(
        einsum("nhd,nhe->hde", query_decay, d_retained),
        True,
        dot(d_attended, mixed_rows, tn).astype(BF16),
    )
    part_out = scatter_chips(grad_out)
    d_raw = (einsum("nhe,mhe->hnm", d_retained, value_rows) * decays).astype(BF16)
    d_query = (
        einsum("hnm,mhd->nhd", d_raw, key_rows)
        + einsum("nhe,hde->nhd", d_retained, state) * query_scale
    )
    d_query = d_query.astype(BF16).reshape(rows, heads * key_width)
    d_keys = (
        einsum("hnm,nhd->mhd", d_raw, query_rows)
        + einsum("mhe,hde->mhd", value_rows, later_grad) * key_scale
    )
    d_keys = d_keys.astype(BF16).reshape(rows, heads * key_width)
    d_values = einsum("hnm,nhe->mhe", weighted, d_retained) + einsum(
        "mhd,hde->mhe", key_decay, later_grad
    )
    d_values = d_values.astype(BF16).reshape(rows, heads * value_width)
    d_normed, first = scatter_group(
        dot(d_gate, full_gate, nt)
        + dot(d_query, full_query, nt)
        + dot(d_keys, full_key, nt)
        + dot(d_values, full_value, nt),
        reduce_gradients(
            blocks // 2, 1, turned, (d_gate, d_values), (part_down, part_up), (output,)
        ),
    )
    grad_gate, grad_value, grad_down, grad_up, output = first
    d_tokens_norm, d_gain_one = norm_back(
        d_normed, tokens_own, mean_one, scale_one, gain_one_own, width
    )
    input_grad = (d_hidden + d_tokens_norm).astype(BF16)
    gain = jnp.concatenate([d_gain_one[None], d_gain_two[None], jnp.zeros((6, cols), F32)])
    grad_query, grad_key, grad_out, input_grad, gain = reduce_gradients(
        blocks // 2, 2, turned, (d_query, d_keys), (part_out,), (input_grad,), (gain,)
    )
    return (
        output,
        input_grad.astype(F32),
        gain[0],
        gain[1],
        grad_query,
        grad_key,
        grad_value,
        grad_gate,
        grad_out.T,
        grad_up,
        grad_down.T,
    )


def solution(mesh):
    seq, head = mesh.devices.shape
    finer = Mesh(mesh.devices.reshape(seq // 2, 2, head // 2, 2), ("p", "c", "zh", "zl"))
    seq, head = ("p", "c"), ("zh", "zl")
    by_row, by_column, one = P(seq, head), P(head, seq), P(head)
    in_specs = (
        (by_row, one, one) + (by_row,) * 4 + (by_column, by_row, by_column) + (by_column, by_row)
    )
    out_specs = (by_row, by_row, one, one) + (by_row,) * 4 + (by_column, by_row, by_column)
    return jax.shard_map(
        on_device, mesh=finer, in_specs=in_specs, out_specs=out_specs, check_vma=False
    )
```

```python
import functools

import jax
import jax.numpy as jnp
from jax import lax
from jax.experimental import pallas as pl
from jax.experimental.pallas import tpu as pltpu
from jax.sharding import Mesh
from jax.sharding import PartitionSpec as P

F32 = jnp.float32
BF16 = jnp.bfloat16

SWAP = ((0, 0), (1, 2), (2, 1), (3, 3))
MOVE = ((0, 1), (1, 3), (2, 0), (3, 2))
BACK = ((1, 0), (3, 1), (0, 2), (2, 3))
FLIP = ((0, 1), (1, 0))


def moments(values):
    mean = jnp.mean(values, axis=-1, keepdims=True)
    centered = values - mean
    spread = jnp.mean(centered * centered, axis=-1, keepdims=True)
    return mean, lax.rsqrt(spread + 1e-05)


MESH = pl.DeviceIdType.MESH


def bits_of(count):
    return count.bit_length() - 1


def flipped(index, stride):
    return index + stride * (1 - 2 * lax.rem(lax.div(index, stride), 2))


class Place:
    def __init__(self, chips):
        self.p, self.c = lax.axis_index("p"), lax.axis_index("c")
        self.zh, self.zl = lax.axis_index("zh"), lax.axis_index("zl")
        self.bits = bits_of(chips)
        self.crossed = lax.rem(self.c + self.zh, 2)
        self.core = {"c": 1 - self.c}
        self.high = {"zh": 1 - self.zh}
        self.diagonal = {"c": 1 - self.c, "zh": 1 - self.zh}
        self.low = {"zl": 1 - self.zl}

    def chip(self, bit):
        return {"p": flipped(self.p, 2**bit)}

    def meet(self):
        barrier = pltpu.get_barrier_semaphore()
        partners = [self.core, self.high, self.diagonal, self.low]
        partners += [self.chip(bit) for bit in range(self.bits)]
        for partner in partners:
            pl.semaphore_signal(barrier, inc=1, device_id=partner, device_id_type=MESH)
        pl.semaphore_wait(barrier, len(partners))

    def moved_to(self):
        return {
            "c": self.c + self.crossed * (1 - 2 * self.c),
            "zh": self.zh + (1 - self.crossed) * (1 - 2 * self.zh),
        }


def remote(src, dst, send, recv, device):
    return pltpu.make_async_remote_copy(
        src_ref=src,
        dst_ref=dst,
        send_sem=send,
        recv_sem=recv,
        device_id=device,
        device_id_type=MESH,
    )


class Relabel:
    def __init__(self, place, src, dst, send, recv):
        self.place = place
        self.moved = remote(src, dst, send.at[0], recv.at[0], place.moved_to())
        self.swapped = remote(src, dst, send.at[1], recv.at[1], place.diagonal)
        self.kept = pltpu.make_async_copy(src, dst, recv.at[1])

    def start(self):
        self.moved.start()
        pl.when(self.place.crossed == 1)(self.swapped.start)
        pl.when(self.place.crossed == 0)(self.kept.start)

    def arrive(self):
        self.moved.wait_recv()
        pl.when(self.place.crossed == 1)(self.swapped.wait_recv)
        pl.when(self.place.crossed == 0)(self.kept.wait)

    def finish(self):
        self.moved.wait_send()
        pl.when(self.place.crossed == 1)(self.swapped.wait_send)


class Spread:
    def __init__(self, place, dst, send, recv):
        self.place, self.dst, self.send, self.recv = place, dst, send, recv
        self.orders = [list(range(place.bits)), list(reversed(range(place.bits)))]

    def copy(self, h, step, mask):
        order = self.orders[h]
        block = self.place.p
        for at in range(self.place.bits):
            if mask >> at & 1:
                block = flipped(block, 2 ** order[at])
        ref = self.dst.at[2 * block + h]
        name = mask + 2**step
        return remote(ref, ref, self.send.at[h, name], self.recv.at[h, name], self.place.chip(order[step]))

    def start(self):
        for step in range(self.place.bits):
            for h in range(2):
                self.copy(h, step, 0).start()

    def arrive(self, mask):
        for h in range(2):
            top = bits_of(mask)
            self.copy(h, top, mask - 2**top).wait_recv()
            for step in range(top + 1, self.place.bits):
                self.copy(h, step, mask).start()

    def rest(self, since):
        for mask in range(since, 2**self.place.bits):
            self.arrive(mask)

    def finish(self):
        for h in range(2):
            for mask in range(1, 2**self.place.bits):
                top = bits_of(mask)
                self.copy(h, top, mask - 2**top).wait_send()


class Columns:
    def __init__(self, place, src, full, send, recv):
        self.place = place
        cols = src.shape[1]

        def at(zl, c):
            return full.at[:, pl.ds(pl.multiple_of((2 * c + zl) * cols, cols), cols)]

        own, near = at(place.zl, place.c), at(1 - place.zl, place.c)
        self.own = own
        crossing = at(place.zl, 1 - place.c)
        self.swapped = remote(src, crossing, send.at[0], recv.at[0], place.diagonal)
        self.kept = pltpu.make_async_copy(src, own, recv.at[0])
        self.low = remote(own, own, send.at[1], recv.at[1], place.low)
        self.core = remote(own, own, send.at[2], recv.at[2], place.core)
        self.passed = remote(near, near, send.at[3], recv.at[3], place.core)

    def start(self):
        pl.when(self.place.crossed == 1)(self.swapped.start)
        pl.when(self.place.crossed == 0)(self.kept.start)

    def second(self):
        pl.when(self.place.crossed == 1)(self.swapped.wait_recv)
        pl.when(self.place.crossed == 0)(self.kept.wait)
        self.low.start()
        self.core.start()

    def third(self):
        self.low.wait_recv()
        self.passed.start()

    def finish(self):
        pl.when(self.place.crossed == 1)(self.swapped.wait_send)
        self.low.wait_send()
        self.core.wait_send()
        self.passed.wait_send()


def project_kernel(chips, *refs):
    decay, query, key, value, gate, out, tokens, cotangent = refs[:8]
    results = refs[8:23]
    full_decay, full_query, full_key, full_value, full_gate, full_out = results[:6]
    grad_full, tokens_own, gains, normed, query_rows = results[6:11]
    key_rows, value_rows, gate_pre, stats = results[11:]
    every, weight, zsend, zrecv, send, recv, tsend, trecv, local = refs[23:]
    place = Place(chips)
    place.meet()
    shards = [decay, query, key, value, gate, out]
    fulls = [full_decay, full_query, full_key, full_value, full_gate, full_out]
    slots = [f.at[2 * place.p + place.c] for f in fulls[:5]] + [full_out.at[place.c]]
    labels = [Relabel(place, s, t, zsend.at[i], zrecv.at[i]) for i, (s, t) in enumerate(zip(shards, slots))]
    spreads = [Spread(place, f, send.at[i], recv.at[i]) for i, f in enumerate(fulls[:5])]
    held = Columns(place, tokens, every, tsend.at[0], trecv.at[0])
    grads = Columns(place, cotangent, grad_full, tsend.at[1], trecv.at[1])
    for i in range(4):
        labels[i].start()
    held.start()

    def spread(i):
        labels[i].arrive()
        spreads[i].start()

    count = tokens.shape[0] - 16
    tile = min(128, count)

    def norm():
        gain = every[count : count + 1, :].astype(F32)

        def one(i, carry):
            at = pl.ds(pl.multiple_of(i * tile, tile), tile)
            v = every[at, :].astype(F32)
            mean, scale = moments(v)
            normed[at, :] = ((v - mean) * scale * gain).astype(BF16)
            stats[0, at, :] = jnp.broadcast_to(mean, (tile, 128))
            stats[1, at, :] = jnp.broadcast_to(scale, (tile, 128))
            return carry

        lax.fori_loop(0, count // tile, one, 0)

    step = min(256, count)

    def project(i, rows):
        spreads[i].rest(2)
        full = fulls[i]
        slots, height, columns = full.shape
        held_weight = weight.at[:, :, pl.ds(0, columns)]
        copy = pltpu.make_async_copy(full, held_weight, local.at[0])
        copy.start()
        copy.wait()

        def one(j, carry):
            at = pl.ds(pl.multiple_of(j * step, step), step)
            w = held_weight[...].reshape(slots * height, columns)
            v = jnp.dot(normed[at, :], w, preferred_element_type=F32)
            rows[at, :] = v.astype(rows.dtype)
            return carry

        lax.fori_loop(0, count // step, one, 0)

    spread(0)
    spread(1)
    spread(2)
    spreads[0].arrive(1)
    spreads[1].arrive(1)
    spread(3)
    spreads[2].arrive(1)
    held.second()
    held.core.wait_recv()
    labels[4].start()
    labels[5].start()
    grads.start()
    spreads[3].arrive(1)
    held.third()
    spread(4)
    held.passed.wait_recv()
    norm()
    project(1, query_rows)
    project(2, key_rows)
    labels[5].arrive()
    spreads[4].arrive(1)
    project(3, value_rows)
    grads.second()
    project(4, gate_pre)
    grads.third()
    spreads[0].rest(2)
    grads.core.wait_recv()
    grads.passed.wait_recv()
    keep = [
        pltpu.make_async_copy(held.own, tokens_own, local.at[1]),
        pltpu.make_async_copy(every.at[pl.ds(count, 16)], gains, local.at[2]),
    ]
    for copy in keep:
        copy.start()
    for label in labels:
        label.finish()
    for each in spreads:
        each.finish()
    held.finish()
    grads.finish()
    for copy in keep:
        copy.wait()


def gather_and_project(chips, decay, query, key, value, gate, out, tokens, cotangent):
    shards = [decay, query, key, value, gate, out]
    rows, cols = tokens.shape[0] - 16, tokens.shape[1]
    width = 4 * cols
    slots = 2 * chips
    shape = jax.ShapeDtypeStruct
    vmem = pl.BlockSpec(memory_space=pltpu.VMEM)
    hbm = pl.BlockSpec(memory_space=pl.ANY)
    gathered = [shape((slots, *s.shape), s.dtype) for s in shards[:5]]
    gathered.append(shape((2, *out.shape), out.dtype))
    wide = [query.shape[1], key.shape[1], value.shape[1], gate.shape[1]]
    made = [
        shape((rows, width), BF16),
        shape((tokens.shape[0], cols), BF16),
        shape((16, width), BF16),
        shape((rows, width), BF16),
        shape((rows, wide[0]), BF16),
        shape((rows, wide[1]), BF16),
        shape((rows, wide[2]), BF16),
        shape((rows, wide[3]), F32),
        shape((2, rows, 128), F32),
    ]
    names = 2 ** bits_of(chips)
    dma = pltpu.SemaphoreType.DMA
    flops = 2 * rows * width * sum(wide)
    return pl.pallas_call(
        functools.partial(project_kernel, chips),
        out_shape=gathered + made,
        in_specs=[vmem] * 8,
        out_specs=[hbm] * 9 + [vmem] * 6,
        scratch_shapes=[
            pltpu.VMEM((tokens.shape[0], width), BF16),
            pltpu.VMEM((slots, value.shape[0], value.shape[1]), BF16),
            dma((6, 2)),
            dma((6, 2)),
            dma((5, 2, names)),
            dma((5, 2, names)),
            dma((2, 4)),
            dma((2, 4)),
            dma((3,)),
        ],
        compiler_params=pltpu.CompilerParams(
            collective_id=0, has_side_effects=True, vmem_limit_bytes=60 * 2**20
        ),
        cost_estimate=pl.CostEstimate(flops=flops, bytes_accessed=60 * 2**20, transcendentals=0),
        name="gather_project",
    )(*shards, tokens, cotangent)


def reduce_kernel(chips, count, ready_count, swap_count, gains, *refs):
    refs = list(refs)

    def taken(number):
        front = refs[:number]
        del refs[:number]
        return front

    turned = taken(1)[0] if count else None
    grads, ready, swaps, gain = taken(count), taken(ready_count), taken(swap_count), taken(gains)
    results, totals, swapped_to = taken(count), taken(ready_count), taken(swap_count)
    gain_to = taken(gains)
    parts, arrived, handed = taken(count), taken(count), taken(count)
    ready_handed = taken(ready_count)
    send, recv, zsend, zrecv = taken(4)
    place = Place(chips)
    place.meet()
    bits = place.bits
    orders = [list(range(bits)), list(reversed(range(bits)))]
    back = {
        "c": place.c + (1 - place.crossed) * (1 - 2 * place.c),
        "zh": place.zh + place.crossed * (1 - 2 * place.zh),
    }

    def slot(h, mask):
        block = place.p
        for at in range(bits):
            if mask >> at & 1:
                block = flipped(block, 2 ** orders[h][at])
        return 2 * block + h

    def added(target, first, second):
        height = first.shape[0]
        step = min(64, height)

        def one(i, carry):
            at = pl.ds(pl.multiple_of(i * step, step), step)
            v = first[at, :].astype(F32) + second[at, :].astype(F32)
            target[at, :] = v.astype(target.dtype)
            return carry

        lax.fori_loop(0, height // step, one, 0)

    def hop(i, h, step, mask):
        name = mask + 2**step
        return remote(
            parts[i].at[slot(h, name)],
            arrived[i].at[h, name],
            send.at[i, h, name],
            recv.at[i, h, name],
            place.chip(orders[h][step]),
        )

    def give(i, step):
        for mask in reversed(range(2**step)):
            for h in range(2):
                hop(i, h, step, mask).start()

    def take(i, step):
        for mask in reversed(range(2**step)):
            for h in range(2):
                hop(i, h, step, mask).wait_recv()
                mine = parts[i].at[slot(h, mask)]
                added(mine, mine, arrived[i].at[h, 2**step + mask])

    def hand(i):
        if i < count:
            even, odd, to = parts[i].at[2 * place.p + 1 - place.zh], own(i), handed[i]
        else:
            even, odd, to = ready[i - count].at[1 - place.zh], own(i), ready_handed[i - count]
        moved = remote(even, to.at[0], zsend.at[i, 0], zrecv.at[i, 0], back)
        swapped = remote(odd, to.at[1], zsend.at[i, 1], zrecv.at[i, 1], place.diagonal)
        return moved, swapped

    def own(i):
        if i < count:
            return parts[i].at[2 * place.p + place.zh]
        return ready[i - count].at[place.zh]

    def hand_out(i):
        moved, swapped = hand(i)
        moved.start()
        pl.when(place.crossed == 1)(swapped.start)

    def settle(i):
        to = handed[i] if i < count else ready_handed[i - count]
        result = results[i] if i < count else totals[i - count]
        moved, swapped = hand(i)
        moved.wait_recv()

        @pl.when(place.crossed == 1)
        def _():
            swapped.wait_recv()
            added(result, to.at[0], to.at[1])

        @pl.when(place.crossed == 0)
        def _():
            added(result, to.at[0], own(i))

    def swapping(i):
        src, dst = swaps[i], swapped_to[i]
        at = count + ready_count + i
        over = remote(src, dst, zsend.at[at, 0], zrecv.at[at, 0], place.diagonal)
        return over, pltpu.make_async_copy(src, dst, zrecv.at[at, 0])

    def multiply(i):
        slots, height, _ = parts[i].shape

        def one(s, carry):
            at = pl.ds(pl.multiple_of(s * height, height), height)
            v = jnp.dot(turned[at, :], grads[i][...], preferred_element_type=F32)
            parts[i][s] = v.astype(BF16)
            return carry

        lax.fori_loop(0, slots, one, 0)

    def stage(i, at):
        if at == 0:
            multiply(i)
            give(i, bits - 1)
        elif at < bits:
            take(i, bits - at)
            give(i, bits - at - 1)
        elif at == bits:
            take(i, 0)
            hand_out(i)
        else:
            settle(i)

    for i in range(ready_count):
        hand_out(count + i)
    for i in range(swap_count):
        over, kept = swapping(i)
        pl.when(place.crossed == 1)(over.start)
        pl.when(place.crossed == 0)(kept.start)
    if gains:
        steps, landed, gsend, grecv = taken(4)
        partners = [place.high] + [place.chip(bit) for bit in range(bits)]

        def step(k):
            return remote(steps.at[k], landed.at[k], gsend.at[k], grecv.at[k], partners[k])

        over = remote(steps.at[bits + 1], gain_to[0], gsend.at[bits + 1], grecv.at[bits + 1], place.diagonal)
        kept = pltpu.make_async_copy(steps.at[bits + 1], gain_to[0], grecv.at[bits + 1])
        steps[0] = gain[0][...]
        step(0).start()
    for tick in range(count + bits + 1):
        for at in range(bits + 2):
            if 0 <= tick - at < count:
                stage(tick - at, at)
    if gains:
        for k in range(bits + 1):
            step(k).wait_recv()
            steps[k + 1] = steps[k] + landed[k]
            if k < bits:
                step(k + 1).start()
        pl.when(place.crossed == 1)(over.start)
        pl.when(place.crossed == 0)(kept.start)
    for i in range(ready_count):
        settle(count + i)
    for i in range(count):
        for h in range(2):
            for at in range(bits):
                for mask in range(2**at):
                    hop(i, h, at, mask).wait_send()
    for i in range(count + ready_count):
        moved, swapped = hand(i)
        moved.wait_send()
        pl.when(place.crossed == 1)(swapped.wait_send)
    if gains:
        for k in range(bits + 1):
            step(k).wait_send()
        pl.when(place.crossed == 1)(over.wait)
        pl.when(place.crossed == 0)(kept.wait)
    for i in range(swap_count):
        over, kept = swapping(i)
        pl.when(place.crossed == 1)(over.wait)
        pl.when(place.crossed == 0)(kept.wait)


def reduce_gradients(chips, identity, turned, grads, ready=(), swaps=(), gain=()):
    count = len(grads)
    slots = 2 * chips
    vmem = pl.BlockSpec(memory_space=pltpu.VMEM)
    wide = [g.shape[1] for g in grads]
    inputs = ([turned] if count else []) + [*grads, *ready, *swaps, *gain]
    height = turned.shape[0] // slots
    named = max(count, 1)
    shape = jax.ShapeDtypeStruct
    dma = pltpu.SemaphoreType.DMA
    moves = count + len(ready) + len(swaps)
    hops = bits_of(chips) + 2
    extra = []
    if gain:
        extra = [pltpu.VMEM((hops, *gain[0].shape), F32)] * 2 + [dma((hops,)), dma((hops,))]
    results = pl.pallas_call(
        functools.partial(reduce_kernel, chips, count, len(ready), len(swaps), len(gain)),
        out_shape=[shape((height, w), F32) for w in wide]
        + [shape(r.shape[1:], F32) for r in ready]
        + [shape(v.shape, v.dtype) for v in (*swaps, *gain)],
        in_specs=[vmem] * len(inputs),
        out_specs=[vmem] * (moves + len(gain)),
        scratch_shapes=[pltpu.VMEM((slots, height, w), BF16) for w in wide]
        + [pltpu.VMEM((2, chips, height, w), BF16) for w in wide]
        + [pltpu.VMEM((2, height, w), BF16) for w in wide]
        + [pltpu.VMEM(r.shape, BF16) for r in ready]
        + [dma((named, 2, chips)), dma((named, 2, chips)), dma((moves, 2)), dma((moves, 2))]
        + extra,
        compiler_params=pltpu.CompilerParams(
            collective_id=identity, has_side_effects=True, vmem_limit_bytes=60 * 2**20
        ),
        cost_estimate=pl.CostEstimate(
            flops=2 * turned.size * sum(wide), bytes_accessed=60 * 2**20, transcendentals=0
        ),
        name=f"reduce_gradients_{identity}",
    )(*inputs)
    return results


def swap(v):
    return lax.ppermute(v, ("c", "zh"), SWAP)


def ordered(first, second, flag, axis):
    return jnp.where(
        flag == 0,
        jnp.concatenate([first, second], axis),
        jnp.concatenate([second, first], axis),
    )


def gather_group(v, fill=()):
    far, fill = lax.optimization_barrier((lax.ppermute(v, "zl", FLIP), fill))
    near = ordered(v, far, lax.axis_index("zl"), 1)
    return ordered(near, lax.ppermute(near, "c", FLIP), lax.axis_index("c"), 1), fill


def half(v, which):
    size = v.shape[1] // 2
    return lax.dynamic_slice_in_dim(v, which * size, size, 1)


def scatter_group(v, fill=()):
    c, zl = lax.axis_index("c"), lax.axis_index("zl")
    far = lax.ppermute(half(v, 1 - c).astype(BF16), "c", FLIP)
    v = half(v, c) + far.astype(F32)
    far = lax.ppermute(half(v, 1 - zl).astype(BF16), "zl", FLIP)
    far, fill = lax.optimization_barrier((far, fill))
    return half(v, zl) + far.astype(F32), fill


def sum_group(v):
    v = v + lax.ppermute(v, "c", FLIP)
    return v + lax.ppermute(v, "zl", FLIP)


def gather_weight(w, axis):
    moved = lax.ppermute(w, ("c", "zh"), MOVE)
    swapped = swap(w)
    pair = ordered(swapped, moved, lax.axis_index("zh"), axis)
    return lax.all_gather(pair, "p", axis=axis, tiled=True)


def scatter_chips(g):
    part = lax.psum_scatter(g, "p", scatter_dimension=0, tiled=True)
    return part.reshape(2, -1, part.shape[1])


def group_norm(values):
    mean, scale = moments(values)
    return (values - mean) * scale


def gelu_tanh(values):
    return jax.nn.gelu(values, approximate=True)


def gated(gate_pre, grouped):
    return jax.nn.silu(gate_pre) * grouped


def decay_weights(running):
    span = running.shape[1]
    gap = running[:, :, None] - running[:, None, :]
    lower = jnp.arange(span)[:, None] >= jnp.arange(span)[None, :]
    return jnp.where(lower[None], jnp.exp(jnp.minimum(gap, 0.0)), 0.0)


def dot(a, b, dims):
    return lax.dot_general(a, b, (dims, ((), ())), preferred_element_type=F32)


def norm_back(d, low, mean, scale, gain, width):
    hat = (low.astype(F32) - mean) * scale
    scaled = d * gain
    sums = sum_group(jnp.stack([jnp.sum(scaled, 1), jnp.sum(scaled * hat, 1)])) / width
    d_in = scale * (scaled - sums[0][:, None] - hat * sums[1][:, None])
    return d_in, jnp.sum(d * hat, 0)


def on_device(
    tokens,
    gain_attn,
    gain_ffn,
    w_query,
    w_key,
    w_value,
    w_gate,
    w_out,
    w_up,
    w_down,
    log_decay,
    cotangent,
):
    rows = tokens.shape[0]
    heads = log_decay.shape[0]
    cols = tokens.shape[1]
    block = 2 * lax.axis_index("p") + lax.axis_index("zh")
    blocks = 2 * lax.axis_size("p")

    extra = jnp.stack([gain_attn, gain_ffn])
    tokens = jnp.concatenate([tokens, jnp.pad(extra, ((0, 14), (0, 0)))])
    decay = jnp.pad(log_decay, ((0, 8 - heads), (0, 0)))
    gathered = gather_and_project(
        blocks // 2, decay, w_query, w_key, w_value, w_gate, w_out.T, tokens, cotangent
    )
    full_decay, full_query, full_key, full_value, full_gate, full_out = gathered[:6]
    grad_full, tokens_own, gains, normed, query_rows = gathered[6:11]
    key_rows, value_rows, gate_pre, stats = gathered[11:]
    quarter = 2 * lax.axis_index("c") + lax.axis_index("zl")
    grad_own = lax.dynamic_slice_in_dim(grad_full, quarter * cols, cols, 1)
    full_query, full_key, full_value, full_gate, full_out = (
        f.reshape(-1, f.shape[2]) for f in (full_query, full_key, full_value, full_gate, full_out)
    )
    full_out = lax.all_gather(full_out, "p", axis=0, tiled=True)
    full_up = gather_weight(w_up, 0)
    full_down = gather_weight(w_down.T, 0)
    width = normed.shape[1]
    key_width = full_query.shape[1] // heads
    value_width = full_value.shape[1] // heads
    gain_two = gains[1].astype(F32)
    gain_one_own, gain_two_own = tokens_own[rows].astype(F32), tokens_own[rows + 1].astype(F32)
    tokens_own = tokens_own[:rows]
    mean_one, scale_one = stats[0, :, :1], stats[1, :, :1]
    block_sums = jnp.sum(full_decay[:, :heads], axis=2)
    log_decay = lax.dynamic_index_in_dim(full_decay, block, 0, False)[:heads]

    nn = ((1,), (0,))
    nt = ((1,), (1,))
    tn = ((0,), (0,))
    query_rows = query_rows.reshape(rows, heads, key_width)
    key_rows = key_rows.reshape(rows, heads, key_width)
    value_rows = value_rows.reshape(rows, heads, value_width)
    running = jnp.cumsum(log_decay, axis=1)
    block_decay = running[:, -1]
    query_scale = jnp.exp(running).T[:, :, None]
    key_scale = jnp.exp(block_decay[:, None] - running).T[:, :, None]
    key_decay = (key_rows * key_scale).astype(BF16)
    query_decay = (query_rows * query_scale).astype(BF16)

    def einsum(spec, a, b):
        return jnp.einsum(spec, a, b, preferred_element_type=F32)

    place = jnp.arange(blocks)[:, None]

    def decay_over(first, last):
        inside = (place >= first) & (place < last)
        return jnp.exp(jnp.sum(jnp.where(inside, block_sums, 0.0), axis=0))[:, None, None]

    def exchanged(v, stride):
        if stride == 1:
            return lax.ppermute(v, "zh", FLIP)
        pairs = [(i, i ^ (stride // 2)) for i in range(blocks // 2)]
        return lax.ppermute(v, "p", pairs)

    def carried(part, backward, fill=(), late=()):
        total, carry = part, jnp.zeros_like(part)
        stride = 1
        while stride < blocks:
            middle = block // (2 * stride) * (2 * stride) + stride
            high = block >= middle
            low_decay = decay_over(middle - stride, middle)
            high_decay = decay_over(middle, middle + stride)
            other = exchanged(total.astype(BF16), stride)
            if stride == 1:
                other, fill = lax.optimization_barrier((other, fill))
            else:
                other, late = lax.optimization_barrier((other, late))
            other = other.astype(F32)
            if backward:
                carry = jnp.where(high, carry, carry + decay_over(block + 1, middle) * other)
                total = jnp.where(high, other + low_decay * total, total + low_decay * other)
            else:
                carry = jnp.where(high, carry + decay_over(middle, block) * other, carry)
                total = jnp.where(high, high_decay * other + total, high_decay * total + other)
            stride *= 2
        return carry.astype(BF16), fill, late

    state, _, _ = carried(einsum("nhd,nhe->hde", key_decay, value_rows), False)
    decays = decay_weights(running)
    weighted = (einsum("nhd,mhd->hnm", query_rows, key_rows) * decays).astype(BF16)
    retained = einsum("hnm,mhe->hne", weighted, value_rows) + einsum(
        "nhd,hde->hne", query_decay, state
    )
    grouped = group_norm(retained)
    grouped = jnp.concatenate([grouped[h] for h in range(heads)], 1)
    mixed_rows = gated(gate_pre, grouped).astype(BF16)
    attended, turned = scatter_group(dot(mixed_rows, full_out, nt), normed.T)
    hidden = tokens_own.astype(F32) + attended
    hidden_own = hidden.astype(BF16)
    hidden_full, d_act = gather_group(hidden_own, dot(grad_full, full_down, nn))
    hidden_full = hidden_full.astype(F32)
    mean_two, scale_two = moments(hidden_full)
    normed_ffn = ((hidden_full - mean_two) * scale_two * gain_two).astype(BF16)
    pre_act = dot(normed_ffn, full_up, nn)
    activated, gelu_back = jax.vjp(gelu_tanh, pre_act)
    activated = activated.astype(BF16)
    d_pre = gelu_back(d_act)[0].astype(BF16)
    d_normed_ffn, grad_down = scatter_group(
        dot(d_pre, full_up, nt), dot(grad_full, activated, tn).astype(BF16)
    )
    part_down = scatter_chips(grad_down)
    d_hidden_norm, d_gain_two = norm_back(
        d_normed_ffn, hidden_own, mean_two, scale_two, gain_two_own, width
    )
    d_hidden = grad_own.astype(F32) + d_hidden_norm
    d_attended, grad_up = gather_group(
        d_hidden.astype(BF16), dot(normed_ffn, d_pre, tn).astype(BF16)
    )
    part_up = scatter_chips(grad_up)
    d_mixed = dot(d_attended, full_out, nn)
    _, gate_back = jax.vjp(gated, gate_pre, grouped)
    d_gate, d_grouped = gate_back(d_mixed)
    d_gate = d_gate.astype(BF16)
    _, group_back = jax.vjp(group_norm, retained)
    d_grouped = jnp.stack(
        [d_grouped[:, h * value_width : (h + 1) * value_width] for h in range(heads)]
    )
    ffn, d_retained = scatter_group(
        dot(activated, full_down, nt), group_back(d_grouped)[0].astype(BF16)
    )
    output = swap((hidden + ffn).astype(BF16))
    later_grad, grad_out, output = carried(
        einsum("nhd,hne->hde", query_decay, d_retained),
        True,
        dot(d_attended, mixed_rows, tn).astype(BF16),
        output,
    )
    part_out = scatter_chips(grad_out)
    d_raw = (einsum("hne,mhe->hnm", d_retained, value_rows) * decays).astype(BF16)
    d_query = (
        einsum("hnm,mhd->nhd", d_raw, key_rows)
        + einsum("hne,hde->nhd", d_retained, state) * query_scale
    )
    d_query = d_query.astype(BF16).reshape(rows, heads * key_width)
    d_keys = (
        einsum("hnm,nhd->mhd", d_raw, query_rows)
        + einsum("mhe,hde->mhd", value_rows, later_grad) * key_scale
    )
    d_keys = d_keys.astype(BF16).reshape(rows, heads * key_width)
    d_values = einsum("hnm,hne->mhe", weighted, d_retained) + einsum(
        "mhd,hde->mhe", key_decay, later_grad
    )
    d_values = d_values.astype(BF16).reshape(rows, heads * value_width)
    d_normed, first = scatter_group(
        dot(d_gate, full_gate, nt)
        + dot(d_query, full_query, nt)
        + dot(d_keys, full_key, nt)
        + dot(d_values, full_value, nt),
        reduce_gradients(
            blocks // 2, 1, turned, (d_query, d_values, d_gate, d_keys), (part_down, part_up)
        ),
    )
    grad_query, grad_value, grad_gate, grad_key, grad_down, grad_up = first
    d_tokens_norm, d_gain_one = norm_back(
        d_normed, tokens_own, mean_one, scale_one, gain_one_own, width
    )
    input_grad = (d_hidden + d_tokens_norm).astype(BF16)
    gain = jnp.concatenate([d_gain_one[None], d_gain_two[None], jnp.zeros((6, cols), F32)])
    grad_out, input_grad, gain = reduce_gradients(
        blocks // 2, 2, turned, (), (part_out,), (input_grad,), (gain,)
    )
    return (
        output,
        input_grad.astype(F32),
        gain[0],
        gain[1],
        grad_query,
        grad_key,
        grad_value,
        grad_gate,
        grad_out.T,
        grad_up,
        grad_down.T,
    )


def solution(mesh):
    seq, head = mesh.devices.shape
    finer = Mesh(mesh.devices.reshape(seq // 2, 2, head // 2, 2), ("p", "c", "zh", "zl"))
    seq, head = ("p", "c"), ("zh", "zl")
    by_row, by_column, one = P(seq, head), P(head, seq), P(head)
    in_specs = (
        (by_row, one, one) + (by_row,) * 4 + (by_column, by_row, by_column) + (by_column, by_row)
    )
    out_specs = (by_row, by_row, one, one) + (by_row,) * 4 + (by_column, by_row, by_column)
    return jax.shard_map(
        on_device, mesh=finer, in_specs=in_specs, out_specs=out_specs, check_vma=False
    )
```

```python
import functools

import jax
import jax.numpy as jnp
from jax import lax
from jax.experimental import pallas as pl
from jax.experimental.pallas import tpu as pltpu
from jax.sharding import Mesh
from jax.sharding import PartitionSpec as P

F32 = jnp.float32
BF16 = jnp.bfloat16

SWAP = ((0, 0), (1, 2), (2, 1), (3, 3))
MOVE = ((0, 1), (1, 3), (2, 0), (3, 2))
BACK = ((1, 0), (3, 1), (0, 2), (2, 3))
FLIP = ((0, 1), (1, 0))


def moments(values):
    mean = jnp.mean(values, axis=-1, keepdims=True)
    centered = values - mean
    spread = jnp.mean(centered * centered, axis=-1, keepdims=True)
    return mean, lax.rsqrt(spread + 1e-05)


MESH = pl.DeviceIdType.MESH


def bits_of(count):
    return count.bit_length() - 1


def flipped(index, stride):
    return index + stride * (1 - 2 * lax.rem(lax.div(index, stride), 2))


class Place:
    def __init__(self, chips):
        self.p, self.c = lax.axis_index("p"), lax.axis_index("c")
        self.zh, self.zl = lax.axis_index("zh"), lax.axis_index("zl")
        self.bits = bits_of(chips)
        self.crossed = lax.rem(self.c + self.zh, 2)
        self.core = {"c": 1 - self.c}
        self.high = {"zh": 1 - self.zh}
        self.diagonal = {"c": 1 - self.c, "zh": 1 - self.zh}
        self.low = {"zl": 1 - self.zl}

    def chip(self, bit):
        return {"p": flipped(self.p, 2**bit)}

    def meet(self):
        barrier = pltpu.get_barrier_semaphore()
        partners = [self.core, self.high, self.diagonal, self.low]
        partners += [self.chip(bit) for bit in range(self.bits)]
        for partner in partners:
            pl.semaphore_signal(barrier, inc=1, device_id=partner, device_id_type=MESH)
        pl.semaphore_wait(barrier, len(partners))

    def moved_to(self):
        return {
            "c": self.c + self.crossed * (1 - 2 * self.c),
            "zh": self.zh + (1 - self.crossed) * (1 - 2 * self.zh),
        }


def remote(src, dst, send, recv, device):
    return pltpu.make_async_remote_copy(
        src_ref=src,
        dst_ref=dst,
        send_sem=send,
        recv_sem=recv,
        device_id=device,
        device_id_type=MESH,
    )


class Relabel:
    def __init__(self, place, src, dst, send, recv):
        self.place = place
        self.moved = remote(src, dst, send.at[0], recv.at[0], place.moved_to())
        self.swapped = remote(src, dst, send.at[1], recv.at[1], place.diagonal)
        self.kept = pltpu.make_async_copy(src, dst, recv.at[1])

    def start(self):
        self.moved.start()
        pl.when(self.place.crossed == 1)(self.swapped.start)
        pl.when(self.place.crossed == 0)(self.kept.start)

    def arrive(self):
        self.moved.wait_recv()
        pl.when(self.place.crossed == 1)(self.swapped.wait_recv)
        pl.when(self.place.crossed == 0)(self.kept.wait)

    def finish(self):
        self.moved.wait_send()
        pl.when(self.place.crossed == 1)(self.swapped.wait_send)


class Spread:
    def __init__(self, place, dst, send, recv):
        self.place, self.dst, self.send, self.recv = place, dst, send, recv
        self.orders = [list(range(place.bits)), list(reversed(range(place.bits)))]

    def copy(self, h, step, mask):
        order = self.orders[h]
        block = self.place.p
        for at in range(self.place.bits):
            if mask >> at & 1:
                block = flipped(block, 2 ** order[at])
        ref = self.dst.at[2 * block + h]
        name = mask + 2**step
        return remote(ref, ref, self.send.at[h, name], self.recv.at[h, name], self.place.chip(order[step]))

    def start(self):
        for step in range(self.place.bits):
            for h in range(2):
                self.copy(h, step, 0).start()

    def arrive(self, mask):
        for h in range(2):
            top = bits_of(mask)
            self.copy(h, top, mask - 2**top).wait_recv()
            for step in range(top + 1, self.place.bits):
                self.copy(h, step, mask).start()

    def rest(self, since):
        for mask in range(since, 2**self.place.bits):
            self.arrive(mask)

    def finish(self):
        for h in range(2):
            for mask in range(1, 2**self.place.bits):
                top = bits_of(mask)
                self.copy(h, top, mask - 2**top).wait_send()


class Columns:
    def __init__(self, place, src, full, send, recv):
        self.place = place
        cols = src.shape[1]

        def at(zl, c):
            return full.at[:, pl.ds(pl.multiple_of((2 * c + zl) * cols, cols), cols)]

        own, near = at(place.zl, place.c), at(1 - place.zl, place.c)
        self.own = own
        crossing = at(place.zl, 1 - place.c)
        self.swapped = remote(src, crossing, send.at[0], recv.at[0], place.diagonal)
        self.kept = pltpu.make_async_copy(src, own, recv.at[0])
        self.low = remote(own, own, send.at[1], recv.at[1], place.low)
        self.core = remote(own, own, send.at[2], recv.at[2], place.core)
        self.passed = remote(near, near, send.at[3], recv.at[3], place.core)

    def start(self):
        pl.when(self.place.crossed == 1)(self.swapped.start)
        pl.when(self.place.crossed == 0)(self.kept.start)

    def second(self):
        pl.when(self.place.crossed == 1)(self.swapped.wait_recv)
        pl.when(self.place.crossed == 0)(self.kept.wait)
        self.low.start()
        self.core.start()

    def third(self):
        self.low.wait_recv()
        self.passed.start()

    def finish(self):
        pl.when(self.place.crossed == 1)(self.swapped.wait_send)
        self.low.wait_send()
        self.core.wait_send()
        self.passed.wait_send()


def project_kernel(chips, *refs):
    decay, query, key, value, gate, out, tokens, cotangent = refs[:8]
    results = refs[8:23]
    full_decay, full_query, full_key, full_value, full_gate, full_out = results[:6]
    grad_full, tokens_own, gains, normed, query_rows = results[6:11]
    key_rows, value_rows, gate_pre, stats = results[11:]
    every, weight, zsend, zrecv, send, recv, tsend, trecv, local = refs[23:]
    place = Place(chips)
    place.meet()
    shards = [decay, query, key, value, gate, out]
    fulls = [full_decay, full_query, full_key, full_value, full_gate, full_out]
    slots = [f.at[2 * place.p + place.c] for f in fulls[:5]] + [full_out.at[place.c]]
    labels = [Relabel(place, s, t, zsend.at[i], zrecv.at[i]) for i, (s, t) in enumerate(zip(shards, slots))]
    spreads = [Spread(place, f, send.at[i], recv.at[i]) for i, f in enumerate(fulls[:5])]
    held = Columns(place, tokens, every, tsend.at[0], trecv.at[0])
    grads = Columns(place, cotangent, grad_full, tsend.at[1], trecv.at[1])
    for i in range(4):
        labels[i].start()
    held.start()

    def spread(i):
        labels[i].arrive()
        spreads[i].start()

    count = tokens.shape[0] - 16
    tile = min(128, count)

    def norm():
        gain = every[count : count + 1, :].astype(F32)

        def one(i, carry):
            at = pl.ds(pl.multiple_of(i * tile, tile), tile)
            v = every[at, :].astype(F32)
            mean, scale = moments(v)
            normed[at, :] = ((v - mean) * scale * gain).astype(BF16)
            stats[0, at, :] = jnp.broadcast_to(mean, (tile, 128))
            stats[1, at, :] = jnp.broadcast_to(scale, (tile, 128))
            return carry

        lax.fori_loop(0, count // tile, one, 0)

    step = min(256, count)

    def project(i, rows):
        spreads[i].rest(2)
        full = fulls[i]
        slots, height, columns = full.shape
        held_weight = weight.at[:, :, pl.ds(0, columns)]
        copy = pltpu.make_async_copy(full, held_weight, local.at[0])
        copy.start()
        copy.wait()

        def one(j, carry):
            at = pl.ds(pl.multiple_of(j * step, step), step)
            w = held_weight[...].reshape(slots * height, columns)
            v = jnp.dot(normed[at, :], w, preferred_element_type=F32)
            rows[at, :] = v.astype(rows.dtype)
            return carry

        lax.fori_loop(0, count // step, one, 0)

    spread(0)
    spread(1)
    spread(2)
    spreads[0].arrive(1)
    spreads[1].arrive(1)
    spread(3)
    spreads[2].arrive(1)
    held.second()
    held.core.wait_recv()
    labels[4].start()
    labels[5].start()
    grads.start()
    spreads[3].arrive(1)
    held.third()
    spread(4)
    held.passed.wait_recv()
    norm()
    project(1, query_rows)
    project(2, key_rows)
    labels[5].arrive()
    spreads[4].arrive(1)
    project(3, value_rows)
    grads.second()
    project(4, gate_pre)
    grads.third()
    spreads[0].rest(2)
    grads.core.wait_recv()
    grads.passed.wait_recv()
    keep = [
        pltpu.make_async_copy(held.own, tokens_own, local.at[1]),
        pltpu.make_async_copy(every.at[pl.ds(count, 16)], gains, local.at[2]),
    ]
    for copy in keep:
        copy.start()
    for label in labels:
        label.finish()
    for each in spreads:
        each.finish()
    held.finish()
    grads.finish()
    for copy in keep:
        copy.wait()


def gather_and_project(chips, decay, query, key, value, gate, out, tokens, cotangent):
    shards = [decay, query, key, value, gate, out]
    rows, cols = tokens.shape[0] - 16, tokens.shape[1]
    width = 4 * cols
    slots = 2 * chips
    shape = jax.ShapeDtypeStruct
    vmem = pl.BlockSpec(memory_space=pltpu.VMEM)
    hbm = pl.BlockSpec(memory_space=pl.ANY)
    gathered = [shape((slots, *s.shape), s.dtype) for s in shards[:5]]
    gathered.append(shape((2, *out.shape), out.dtype))
    wide = [query.shape[1], key.shape[1], value.shape[1], gate.shape[1]]
    made = [
        shape((rows, width), BF16),
        shape((tokens.shape[0], cols), BF16),
        shape((16, width), BF16),
        shape((rows, width), BF16),
        shape((rows, wide[0]), BF16),
        shape((rows, wide[1]), BF16),
        shape((rows, wide[2]), BF16),
        shape((rows, wide[3]), F32),
        shape((2, rows, 128), F32),
    ]
    names = 2 ** bits_of(chips)
    dma = pltpu.SemaphoreType.DMA
    flops = 2 * rows * width * sum(wide)
    return pl.pallas_call(
        functools.partial(project_kernel, chips),
        out_shape=gathered + made,
        in_specs=[vmem] * 8,
        out_specs=[hbm] * 9 + [vmem] * 6,
        scratch_shapes=[
            pltpu.VMEM((tokens.shape[0], width), BF16),
            pltpu.VMEM((slots, value.shape[0], value.shape[1]), BF16),
            dma((6, 2)),
            dma((6, 2)),
            dma((5, 2, names)),
            dma((5, 2, names)),
            dma((2, 4)),
            dma((2, 4)),
            dma((3,)),
        ],
        compiler_params=pltpu.CompilerParams(
            collective_id=0, has_side_effects=True, vmem_limit_bytes=60 * 2**20
        ),
        cost_estimate=pl.CostEstimate(flops=flops, bytes_accessed=60 * 2**20, transcendentals=0),
        name="gather_project",
    )(*shards, tokens, cotangent)


def reduce_kernel(chips, count, ready_count, swap_count, gains, *refs):
    refs = list(refs)

    def taken(number):
        front = refs[:number]
        del refs[:number]
        return front

    turned = taken(1)[0] if count else None
    grads, ready, swaps, gain = taken(count), taken(ready_count), taken(swap_count), taken(gains)
    results, totals, swapped_to = taken(count), taken(ready_count), taken(swap_count)
    gain_to = taken(gains)
    parts, arrived, handed = taken(count), taken(count), taken(count)
    ready_handed = taken(ready_count)
    send, recv, zsend, zrecv = taken(4)
    place = Place(chips)
    place.meet()
    bits = place.bits
    orders = [list(range(bits)), list(reversed(range(bits)))]
    back = {
        "c": place.c + (1 - place.crossed) * (1 - 2 * place.c),
        "zh": place.zh + place.crossed * (1 - 2 * place.zh),
    }

    def slot(h, mask):
        block = place.p
        for at in range(bits):
            if mask >> at & 1:
                block = flipped(block, 2 ** orders[h][at])
        return 2 * block + h

    def added(target, first, second):
        height = first.shape[0]
        step = min(64, height)

        def one(i, carry):
            at = pl.ds(pl.multiple_of(i * step, step), step)
            v = first[at, :].astype(F32) + second[at, :].astype(F32)
            target[at, :] = v.astype(target.dtype)
            return carry

        lax.fori_loop(0, height // step, one, 0)

    def hop(i, h, step, mask):
        name = mask + 2**step
        return remote(
            parts[i].at[slot(h, name)],
            arrived[i].at[h, name],
            send.at[i, h, name],
            recv.at[i, h, name],
            place.chip(orders[h][step]),
        )

    def give(i, step):
        for mask in reversed(range(2**step)):
            for h in range(2):
                hop(i, h, step, mask).start()

    def take(i, step):
        for mask in reversed(range(2**step)):
            for h in range(2):
                hop(i, h, step, mask).wait_recv()
                mine = parts[i].at[slot(h, mask)]
                added(mine, mine, arrived[i].at[h, 2**step + mask])

    def hand(i):
        if i < count:
            even, odd, to = parts[i].at[2 * place.p + 1 - place.zh], own(i), handed[i]
        else:
            even, odd, to = ready[i - count].at[1 - place.zh], own(i), ready_handed[i - count]
        moved = remote(even, to.at[0], zsend.at[i, 0], zrecv.at[i, 0], back)
        swapped = remote(odd, to.at[1], zsend.at[i, 1], zrecv.at[i, 1], place.diagonal)
        return moved, swapped

    def own(i):
        if i < count:
            return parts[i].at[2 * place.p + place.zh]
        return ready[i - count].at[place.zh]

    def hand_out(i):
        moved, swapped = hand(i)
        moved.start()
        pl.when(place.crossed == 1)(swapped.start)

    def settle(i):
        to = handed[i] if i < count else ready_handed[i - count]
        result = results[i] if i < count else totals[i - count]
        moved, swapped = hand(i)
        moved.wait_recv()

        @pl.when(place.crossed == 1)
        def _():
            swapped.wait_recv()
            added(result, to.at[0], to.at[1])

        @pl.when(place.crossed == 0)
        def _():
            added(result, to.at[0], own(i))

    def swapping(i):
        src, dst = swaps[i], swapped_to[i]
        at = count + ready_count + i
        over = remote(src, dst, zsend.at[at, 0], zrecv.at[at, 0], place.diagonal)
        return over, pltpu.make_async_copy(src, dst, zrecv.at[at, 0])

    def multiply(i):
        slots, height, _ = parts[i].shape

        def one(s, carry):
            at = pl.ds(pl.multiple_of(s * height, height), height)
            v = jnp.dot(turned[at, :], grads[i][...], preferred_element_type=F32)
            parts[i][s] = v.astype(BF16)
            return carry

        lax.fori_loop(0, slots, one, 0)

    def stage(i, at):
        if at == 0:
            multiply(i)
            give(i, bits - 1)
        elif at < bits:
            take(i, bits - at)
            give(i, bits - at - 1)
        elif at == bits:
            take(i, 0)
            hand_out(i)
        else:
            settle(i)

    for i in range(ready_count):
        hand_out(count + i)
    for i in range(swap_count):
        over, kept = swapping(i)
        pl.when(place.crossed == 1)(over.start)
        pl.when(place.crossed == 0)(kept.start)
    if gains:
        steps, landed, gsend, grecv = taken(4)
        partners = [place.high] + [place.chip(bit) for bit in range(bits)]

        def step(k):
            return remote(steps.at[k], landed.at[k], gsend.at[k], grecv.at[k], partners[k])

        over = remote(steps.at[bits + 1], gain_to[0], gsend.at[bits + 1], grecv.at[bits + 1], place.diagonal)
        kept = pltpu.make_async_copy(steps.at[bits + 1], gain_to[0], grecv.at[bits + 1])
        steps[0] = gain[0][...]
        step(0).start()
    for tick in range(count + bits + 1):
        for at in range(bits + 2):
            if 0 <= tick - at < count:
                stage(tick - at, at)
    if gains:
        for k in range(bits + 1):
            step(k).wait_recv()
            steps[k + 1] = steps[k] + landed[k]
            if k < bits:
                step(k + 1).start()
        pl.when(place.crossed == 1)(over.start)
        pl.when(place.crossed == 0)(kept.start)
    for i in range(ready_count):
        settle(count + i)
    for i in range(count):
        for h in range(2):
            for at in range(bits):
                for mask in range(2**at):
                    hop(i, h, at, mask).wait_send()
    for i in range(count + ready_count):
        moved, swapped = hand(i)
        moved.wait_send()
        pl.when(place.crossed == 1)(swapped.wait_send)
    if gains:
        for k in range(bits + 1):
            step(k).wait_send()
        pl.when(place.crossed == 1)(over.wait)
        pl.when(place.crossed == 0)(kept.wait)
    for i in range(swap_count):
        over, kept = swapping(i)
        pl.when(place.crossed == 1)(over.wait)
        pl.when(place.crossed == 0)(kept.wait)


def reduce_gradients(chips, identity, turned, grads, ready=(), swaps=(), gain=()):
    count = len(grads)
    slots = 2 * chips
    vmem = pl.BlockSpec(memory_space=pltpu.VMEM)
    wide = [g.shape[1] for g in grads]
    inputs = ([turned] if count else []) + [*grads, *ready, *swaps, *gain]
    height = turned.shape[0] // slots
    named = max(count, 1)
    shape = jax.ShapeDtypeStruct
    dma = pltpu.SemaphoreType.DMA
    moves = count + len(ready) + len(swaps)
    hops = bits_of(chips) + 2
    extra = []
    if gain:
        extra = [pltpu.VMEM((hops, *gain[0].shape), F32)] * 2 + [dma((hops,)), dma((hops,))]
    results = pl.pallas_call(
        functools.partial(reduce_kernel, chips, count, len(ready), len(swaps), len(gain)),
        out_shape=[shape((height, w), F32) for w in wide]
        + [shape(r.shape[1:], F32) for r in ready]
        + [shape(v.shape, v.dtype) for v in (*swaps, *gain)],
        in_specs=[vmem] * len(inputs),
        out_specs=[vmem] * (moves + len(gain)),
        scratch_shapes=[pltpu.VMEM((slots, height, w), BF16) for w in wide]
        + [pltpu.VMEM((2, chips, height, w), BF16) for w in wide]
        + [pltpu.VMEM((2, height, w), BF16) for w in wide]
        + [pltpu.VMEM(r.shape, BF16) for r in ready]
        + [dma((named, 2, chips)), dma((named, 2, chips)), dma((moves, 2)), dma((moves, 2))]
        + extra,
        compiler_params=pltpu.CompilerParams(
            collective_id=identity, has_side_effects=True, vmem_limit_bytes=60 * 2**20
        ),
        cost_estimate=pl.CostEstimate(
            flops=2 * turned.size * sum(wide), bytes_accessed=60 * 2**20, transcendentals=0
        ),
        name=f"reduce_gradients_{identity}",
    )(*inputs)
    return results


def swap(v):
    return lax.ppermute(v, ("c", "zh"), SWAP)


def ordered(first, second, flag, axis):
    return jnp.where(
        flag == 0,
        jnp.concatenate([first, second], axis),
        jnp.concatenate([second, first], axis),
    )


def gather_group(v, fill=()):
    far, fill = lax.optimization_barrier((lax.ppermute(v, "zl", FLIP), fill))
    near = ordered(v, far, lax.axis_index("zl"), 1)
    return ordered(near, lax.ppermute(near, "c", FLIP), lax.axis_index("c"), 1), fill


def half(v, which):
    size = v.shape[1] // 2
    return lax.dynamic_slice_in_dim(v, which * size, size, 1)


def scatter_group(v, fill=()):
    c, zl = lax.axis_index("c"), lax.axis_index("zl")
    far = lax.ppermute(half(v, 1 - c).astype(BF16), "c", FLIP)
    v = half(v, c) + far.astype(F32)
    far = lax.ppermute(half(v, 1 - zl).astype(BF16), "zl", FLIP)
    far, fill = lax.optimization_barrier((far, fill))
    return half(v, zl) + far.astype(F32), fill


def sum_group(v):
    v = v + lax.ppermute(v, "c", FLIP)
    return v + lax.ppermute(v, "zl", FLIP)


def gather_weight(w, axis):
    moved = lax.ppermute(w, ("c", "zh"), MOVE)
    swapped = swap(w)
    pair = ordered(swapped, moved, lax.axis_index("zh"), axis)
    return lax.all_gather(pair, "p", axis=axis, tiled=True)


def scatter_chips(g):
    part = lax.psum_scatter(g, "p", scatter_dimension=0, tiled=True)
    return part.reshape(2, -1, part.shape[1])


def group_norm(values):
    mean, scale = moments(values)
    return (values - mean) * scale


def gelu_tanh(values):
    return jax.nn.gelu(values, approximate=True)


def gated(gate_pre, grouped):
    return jax.nn.silu(gate_pre) * grouped


def decay_weights(running):
    span = running.shape[1]
    gap = running[:, :, None] - running[:, None, :]
    lower = jnp.arange(span)[:, None] >= jnp.arange(span)[None, :]
    return jnp.where(lower[None], jnp.exp(jnp.minimum(gap, 0.0)), 0.0)


def dot(a, b, dims):
    return lax.dot_general(a, b, (dims, ((), ())), preferred_element_type=F32)


def norm_back(d, low, mean, scale, gain, width):
    hat = (low.astype(F32) - mean) * scale
    scaled = d * gain
    sums = sum_group(jnp.stack([jnp.sum(scaled, 1), jnp.sum(scaled * hat, 1)])) / width
    d_in = scale * (scaled - sums[0][:, None] - hat * sums[1][:, None])
    return d_in, jnp.sum(d * hat, 0)


def on_device(
    tokens,
    gain_attn,
    gain_ffn,
    w_query,
    w_key,
    w_value,
    w_gate,
    w_out,
    w_up,
    w_down,
    log_decay,
    cotangent,
):
    rows = tokens.shape[0]
    heads = log_decay.shape[0]
    cols = tokens.shape[1]
    block = 2 * lax.axis_index("p") + lax.axis_index("zh")
    blocks = 2 * lax.axis_size("p")

    extra = jnp.stack([gain_attn, gain_ffn])
    tokens = jnp.concatenate([tokens, jnp.pad(extra, ((0, 14), (0, 0)))])
    decay = jnp.pad(log_decay, ((0, 8 - heads), (0, 0)))
    gathered = gather_and_project(
        blocks // 2, decay, w_query, w_key, w_value, w_gate, w_out.T, tokens, cotangent
    )
    full_decay, full_query, full_key, full_value, full_gate, full_out = gathered[:6]
    grad_full, tokens_own, gains, normed, query_rows = gathered[6:11]
    key_rows, value_rows, gate_pre, stats = gathered[11:]
    quarter = 2 * lax.axis_index("c") + lax.axis_index("zl")
    grad_own = lax.dynamic_slice_in_dim(grad_full, quarter * cols, cols, 1)
    full_query, full_key, full_value, full_gate, full_out = (
        f.reshape(-1, f.shape[2]) for f in (full_query, full_key, full_value, full_gate, full_out)
    )
    full_out = lax.all_gather(full_out, "p", axis=0, tiled=True)
    full_up = gather_weight(w_up, 0)
    full_down = gather_weight(w_down.T, 0)
    width = normed.shape[1]
    key_width = full_query.shape[1] // heads
    value_width = full_value.shape[1] // heads
    gain_two = gains[1].astype(F32)
    gain_one_own, gain_two_own = tokens_own[rows].astype(F32), tokens_own[rows + 1].astype(F32)
    tokens_own = tokens_own[:rows]
    mean_one, scale_one = stats[0, :, :1], stats[1, :, :1]
    block_sums = jnp.sum(full_decay[:, :heads], axis=2)
    log_decay = lax.dynamic_index_in_dim(full_decay, block, 0, False)[:heads]

    nn = ((1,), (0,))
    nt = ((1,), (1,))
    tn = ((0,), (0,))
    query_rows = query_rows.reshape(rows, heads, key_width)
    key_rows = key_rows.reshape(rows, heads, key_width)
    value_rows = value_rows.reshape(rows, heads, value_width)
    running = jnp.cumsum(log_decay, axis=1)
    block_decay = running[:, -1]
    query_scale = jnp.exp(running).T[:, :, None]
    key_scale = jnp.exp(block_decay[:, None] - running).T[:, :, None]
    key_decay = (key_rows * key_scale).astype(BF16)
    query_decay = (query_rows * query_scale).astype(BF16)

    def einsum(spec, a, b):
        return jnp.einsum(spec, a, b, preferred_element_type=F32)

    place = jnp.arange(blocks)[:, None]

    def decay_over(first, last):
        inside = (place >= first) & (place < last)
        return jnp.exp(jnp.sum(jnp.where(inside, block_sums, 0.0), axis=0))[:, None, None]

    def exchanged(v, stride):
        if stride == 1:
            return lax.ppermute(v, "zh", FLIP)
        pairs = [(i, i ^ (stride // 2)) for i in range(blocks // 2)]
        return lax.ppermute(v, "p", pairs)

    def carried(part, backward, fill=(), late=()):
        total, carry = part, jnp.zeros_like(part)
        stride = 1
        while stride < blocks:
            middle = block // (2 * stride) * (2 * stride) + stride
            high = block >= middle
            low_decay = decay_over(middle - stride, middle)
            high_decay = decay_over(middle, middle + stride)
            other = exchanged(total.astype(BF16), stride)
            if stride == 1:
                other, fill = lax.optimization_barrier((other, fill))
            else:
                other, late = lax.optimization_barrier((other, late))
            other = other.astype(F32)
            if backward:
                carry = jnp.where(high, carry, carry + decay_over(block + 1, middle) * other)
                total = jnp.where(high, other + low_decay * total, total + low_decay * other)
            else:
                carry = jnp.where(high, carry + decay_over(middle, block) * other, carry)
                total = jnp.where(high, high_decay * other + total, high_decay * total + other)
            stride *= 2
        return carry.astype(BF16), fill, late

    state, _, _ = carried(einsum("nhd,nhe->hde", key_decay, value_rows), False)
    decays = decay_weights(running)
    weighted = (einsum("nhd,mhd->hnm", query_rows, key_rows) * decays).astype(BF16)
    retained = einsum("hnm,mhe->hne", weighted, value_rows) + einsum(
        "nhd,hde->hne", query_decay, state
    )
    grouped = group_norm(retained)
    grouped = jnp.concatenate([grouped[h] for h in range(heads)], 1)
    mixed_rows = gated(gate_pre, grouped).astype(BF16)
    attended, turned = scatter_group(dot(mixed_rows, full_out, nt), normed.T)
    hidden = tokens_own.astype(F32) + attended
    hidden_own = hidden.astype(BF16)
    hidden_full, d_act = gather_group(hidden_own, dot(grad_full, full_down, nn))
    hidden_full = hidden_full.astype(F32)
    mean_two, scale_two = moments(hidden_full)
    normed_ffn = ((hidden_full - mean_two) * scale_two * gain_two).astype(BF16)
    pre_act = dot(normed_ffn, full_up, nn)
    activated, gelu_back = jax.vjp(gelu_tanh, pre_act)
    activated = activated.astype(BF16)
    d_pre = gelu_back(d_act)[0].astype(BF16)
    d_normed_ffn, grad_down = scatter_group(
        dot(d_pre, full_up, nt), dot(grad_full, activated, tn).astype(BF16)
    )
    part_down = scatter_chips(grad_down)
    d_hidden_norm, d_gain_two = norm_back(
        d_normed_ffn, hidden_own, mean_two, scale_two, gain_two_own, width
    )
    d_hidden = grad_own.astype(F32) + d_hidden_norm
    d_attended, grad_up = gather_group(
        d_hidden.astype(BF16), dot(normed_ffn, d_pre, tn).astype(BF16)
    )
    part_up = scatter_chips(grad_up)
    d_mixed = dot(d_attended, full_out, nn)
    _, gate_back = jax.vjp(gated, gate_pre, grouped)
    d_gate, d_grouped = gate_back(d_mixed)
    d_gate = d_gate.astype(BF16)
    _, group_back = jax.vjp(group_norm, retained)
    d_grouped = jnp.stack(
        [d_grouped[:, h * value_width : (h + 1) * value_width] for h in range(heads)]
    )
    ffn, d_retained = scatter_group(
        dot(activated, full_down, nt), group_back(d_grouped)[0].astype(BF16)
    )
    output = swap((hidden + ffn).astype(BF16))
    later_grad, grad_out, output = carried(
        einsum("nhd,hne->hde", query_decay, d_retained),
        True,
        dot(d_attended, mixed_rows, tn).astype(BF16),
        output,
    )
    part_out = scatter_chips(grad_out)
    d_raw = (einsum("hne,mhe->hnm", d_retained, value_rows) * decays).astype(BF16)
    d_query = (
        einsum("hnm,mhd->nhd", d_raw, key_rows)
        + einsum("hne,hde->nhd", d_retained, state) * query_scale
    )
    d_query = d_query.astype(BF16).reshape(rows, heads * key_width)
    d_keys = (
        einsum("hnm,nhd->mhd", d_raw, query_rows)
        + einsum("mhe,hde->mhd", value_rows, later_grad) * key_scale
    )
    d_keys = d_keys.astype(BF16).reshape(rows, heads * key_width)
    d_values = einsum("hnm,hne->mhe", weighted, d_retained) + einsum(
        "mhd,hde->mhe", key_decay, later_grad
    )
    d_values = d_values.astype(BF16).reshape(rows, heads * value_width)
    d_normed, first = scatter_group(
        dot(d_gate, full_gate, nt)
        + dot(d_query, full_query, nt)
        + dot(d_keys, full_key, nt)
        + dot(d_values, full_value, nt),
        reduce_gradients(
            blocks // 2, 1, turned, (d_query, d_values, d_gate, d_keys),
            (part_down, part_up, part_out),
        ),
    )
    grad_query, grad_value, grad_gate, grad_key, grad_down, grad_up, grad_out = first
    d_tokens_norm, d_gain_one = norm_back(
        d_normed, tokens_own, mean_one, scale_one, gain_one_own, width
    )
    input_grad = (d_hidden + d_tokens_norm).astype(BF16)
    gain = jnp.concatenate([d_gain_one[None], d_gain_two[None], jnp.zeros((6, cols), F32)])
    input_grad, gain = reduce_gradients(blocks // 2, 2, turned, (), (), (input_grad,), (gain,))
    return (
        output,
        input_grad.astype(F32),
        gain[0],
        gain[1],
        grad_query,
        grad_key,
        grad_value,
        grad_gate,
        grad_out.T,
        grad_up,
        grad_down.T,
    )


def solution(mesh):
    seq, head = mesh.devices.shape
    finer = Mesh(mesh.devices.reshape(seq // 2, 2, head // 2, 2), ("p", "c", "zh", "zl"))
    seq, head = ("p", "c"), ("zh", "zl")
    by_row, by_column, one = P(seq, head), P(head, seq), P(head)
    in_specs = (
        (by_row, one, one) + (by_row,) * 4 + (by_column, by_row, by_column) + (by_column, by_row)
    )
    out_specs = (by_row, by_row, one, one) + (by_row,) * 4 + (by_column, by_row, by_column)
    return jax.shard_map(
        on_device, mesh=finer, in_specs=in_specs, out_specs=out_specs, check_vma=False
    )
```

```python
import functools

import jax
import jax.numpy as jnp
from jax import lax
from jax.experimental import pallas as pl
from jax.experimental.pallas import tpu as pltpu
from jax.sharding import Mesh
from jax.sharding import PartitionSpec as P

F32 = jnp.float32
BF16 = jnp.bfloat16

SWAP = ((0, 0), (1, 2), (2, 1), (3, 3))
MOVE = ((0, 1), (1, 3), (2, 0), (3, 2))
BACK = ((1, 0), (3, 1), (0, 2), (2, 3))
FLIP = ((0, 1), (1, 0))


def moments(values):
    mean = jnp.mean(values, axis=-1, keepdims=True)
    centered = values - mean
    spread = jnp.mean(centered * centered, axis=-1, keepdims=True)
    return mean, lax.rsqrt(spread + 1e-05)


MESH = pl.DeviceIdType.MESH


def bits_of(count):
    return count.bit_length() - 1


def flipped(index, stride):
    return index + stride * (1 - 2 * lax.rem(lax.div(index, stride), 2))


class Place:
    def __init__(self, chips):
        self.p, self.c = lax.axis_index("p"), lax.axis_index("c")
        self.zh, self.zl = lax.axis_index("zh"), lax.axis_index("zl")
        self.bits = bits_of(chips)
        self.crossed = lax.rem(self.c + self.zh, 2)
        self.core = {"c": 1 - self.c}
        self.high = {"zh": 1 - self.zh}
        self.diagonal = {"c": 1 - self.c, "zh": 1 - self.zh}
        self.low = {"zl": 1 - self.zl}

    def chip(self, bit):
        return {"p": flipped(self.p, 2**bit)}

    def meet(self):
        barrier = pltpu.get_barrier_semaphore()
        partners = [self.core, self.high, self.diagonal, self.low]
        partners += [self.chip(bit) for bit in range(self.bits)]
        for partner in partners:
            pl.semaphore_signal(barrier, inc=1, device_id=partner, device_id_type=MESH)
        pl.semaphore_wait(barrier, len(partners))

    def moved_to(self):
        return {
            "c": self.c + self.crossed * (1 - 2 * self.c),
            "zh": self.zh + (1 - self.crossed) * (1 - 2 * self.zh),
        }


def remote(src, dst, send, recv, device):
    return pltpu.make_async_remote_copy(
        src_ref=src,
        dst_ref=dst,
        send_sem=send,
        recv_sem=recv,
        device_id=device,
        device_id_type=MESH,
    )


class Relabel:
    def __init__(self, place, src, dst, send, recv):
        self.place = place
        self.moved = remote(src, dst, send.at[0], recv.at[0], place.moved_to())
        self.swapped = remote(src, dst, send.at[1], recv.at[1], place.diagonal)
        self.kept = pltpu.make_async_copy(src, dst, recv.at[1])

    def start(self):
        self.moved.start()
        pl.when(self.place.crossed == 1)(self.swapped.start)
        pl.when(self.place.crossed == 0)(self.kept.start)

    def arrive(self):
        self.moved.wait_recv()
        pl.when(self.place.crossed == 1)(self.swapped.wait_recv)
        pl.when(self.place.crossed == 0)(self.kept.wait)

    def finish(self):
        self.moved.wait_send()
        pl.when(self.place.crossed == 1)(self.swapped.wait_send)


class Spread:
    def __init__(self, place, dst, send, recv):
        self.place, self.dst, self.send, self.recv = place, dst, send, recv
        self.orders = [list(range(place.bits)), list(reversed(range(place.bits)))]

    def copy(self, h, step, mask):
        order = self.orders[h]
        block = self.place.p
        for at in range(self.place.bits):
            if mask >> at & 1:
                block = flipped(block, 2 ** order[at])
        ref = self.dst.at[2 * block + h]
        name = mask + 2**step
        return remote(ref, ref, self.send.at[h, name], self.recv.at[h, name], self.place.chip(order[step]))

    def start(self):
        for step in range(self.place.bits):
            for h in range(2):
                self.copy(h, step, 0).start()

    def arrive(self, mask):
        for h in range(2):
            top = bits_of(mask)
            self.copy(h, top, mask - 2**top).wait_recv()
            for step in range(top + 1, self.place.bits):
                self.copy(h, step, mask).start()

    def rest(self, since):
        for mask in range(since, 2**self.place.bits):
            self.arrive(mask)

    def finish(self):
        for h in range(2):
            for mask in range(1, 2**self.place.bits):
                top = bits_of(mask)
                self.copy(h, top, mask - 2**top).wait_send()


class Columns:
    def __init__(self, place, src, full, send, recv):
        self.place = place
        cols = src.shape[1]

        def at(zl, c):
            return full.at[:, pl.ds(pl.multiple_of((2 * c + zl) * cols, cols), cols)]

        own, near = at(place.zl, place.c), at(1 - place.zl, place.c)
        self.own = own
        crossing = at(place.zl, 1 - place.c)
        self.swapped = remote(src, crossing, send.at[0], recv.at[0], place.diagonal)
        self.kept = pltpu.make_async_copy(src, own, recv.at[0])
        self.low = remote(own, own, send.at[1], recv.at[1], place.low)
        self.core = remote(own, own, send.at[2], recv.at[2], place.core)
        self.passed = remote(near, near, send.at[3], recv.at[3], place.core)

    def start(self):
        pl.when(self.place.crossed == 1)(self.swapped.start)
        pl.when(self.place.crossed == 0)(self.kept.start)

    def second(self):
        pl.when(self.place.crossed == 1)(self.swapped.wait_recv)
        pl.when(self.place.crossed == 0)(self.kept.wait)
        self.low.start()
        self.core.start()

    def third(self):
        self.low.wait_recv()
        self.passed.start()

    def finish(self):
        pl.when(self.place.crossed == 1)(self.swapped.wait_send)
        self.low.wait_send()
        self.core.wait_send()
        self.passed.wait_send()


def project_kernel(chips, *refs):
    decay, query, key, value, gate, out, tokens, cotangent = refs[:8]
    results = refs[8:23]
    full_decay, full_query, full_key, full_value, full_gate, full_out = results[:6]
    grad_full, tokens_own, gains, normed, query_rows = results[6:11]
    key_rows, value_rows, gate_pre, stats = results[11:]
    every, weight, zsend, zrecv, send, recv, tsend, trecv, local = refs[23:]
    place = Place(chips)
    place.meet()
    shards = [decay, query, key, value, gate, out]
    fulls = [full_decay, full_query, full_key, full_value, full_gate, full_out]
    slots = [f.at[2 * place.p + place.c] for f in fulls[:5]] + [full_out.at[place.c]]
    labels = [Relabel(place, s, t, zsend.at[i], zrecv.at[i]) for i, (s, t) in enumerate(zip(shards, slots))]
    spreads = [Spread(place, f, send.at[i], recv.at[i]) for i, f in enumerate(fulls[:5])]
    held = Columns(place, tokens, every, tsend.at[0], trecv.at[0])
    grads = Columns(place, cotangent, grad_full, tsend.at[1], trecv.at[1])
    for i in range(4):
        labels[i].start()
    held.start()

    def spread(i):
        labels[i].arrive()
        spreads[i].start()

    count = tokens.shape[0] - 16
    tile = min(128, count)

    def norm():
        gain = every[count : count + 1, :].astype(F32)

        def one(i, carry):
            at = pl.ds(pl.multiple_of(i * tile, tile), tile)
            v = every[at, :].astype(F32)
            mean, scale = moments(v)
            normed[at, :] = ((v - mean) * scale * gain).astype(BF16)
            stats[0, at, :] = jnp.broadcast_to(mean, (tile, 128))
            stats[1, at, :] = jnp.broadcast_to(scale, (tile, 128))
            return carry

        lax.fori_loop(0, count // tile, one, 0)

    step = min(256, count)

    def project(i, rows):
        spreads[i].rest(2)
        full = fulls[i]
        slots, height, columns = full.shape
        held_weight = weight.at[:, :, pl.ds(0, columns)]
        copy = pltpu.make_async_copy(full, held_weight, local.at[0])
        copy.start()
        copy.wait()

        def one(j, carry):
            at = pl.ds(pl.multiple_of(j * step, step), step)
            w = held_weight[...].reshape(slots * height, columns)
            v = jnp.dot(normed[at, :], w, preferred_element_type=F32)
            rows[at, :] = v.astype(rows.dtype)
            return carry

        lax.fori_loop(0, count // step, one, 0)

    spread(0)
    spread(1)
    spread(2)
    spreads[0].arrive(1)
    spreads[1].arrive(1)
    spread(3)
    spreads[2].arrive(1)
    held.second()
    held.core.wait_recv()
    labels[4].start()
    grads.start()
    labels[5].start()
    spreads[3].arrive(1)
    held.third()
    spread(4)
    held.passed.wait_recv()
    norm()
    project(1, query_rows)
    project(2, key_rows)
    spreads[4].arrive(1)
    grads.second()
    project(3, value_rows)
    grads.third()
    project(4, gate_pre)
    spreads[0].rest(2)
    labels[5].arrive()
    grads.core.wait_recv()
    grads.passed.wait_recv()
    keep = [
        pltpu.make_async_copy(held.own, tokens_own, local.at[1]),
        pltpu.make_async_copy(every.at[pl.ds(count, 16)], gains, local.at[2]),
    ]
    for copy in keep:
        copy.start()
    for label in labels:
        label.finish()
    for each in spreads:
        each.finish()
    held.finish()
    grads.finish()
    for copy in keep:
        copy.wait()


def gather_and_project(chips, decay, query, key, value, gate, out, tokens, cotangent):
    shards = [decay, query, key, value, gate, out]
    rows, cols = tokens.shape[0] - 16, tokens.shape[1]
    width = 4 * cols
    slots = 2 * chips
    shape = jax.ShapeDtypeStruct
    vmem = pl.BlockSpec(memory_space=pltpu.VMEM)
    hbm = pl.BlockSpec(memory_space=pl.ANY)
    gathered = [shape((slots, *s.shape), s.dtype) for s in shards[:5]]
    gathered.append(shape((2, *out.shape), out.dtype))
    wide = [query.shape[1], key.shape[1], value.shape[1], gate.shape[1]]
    made = [
        shape((rows, width), BF16),
        shape((tokens.shape[0], cols), BF16),
        shape((16, width), BF16),
        shape((rows, width), BF16),
        shape((rows, wide[0]), BF16),
        shape((rows, wide[1]), BF16),
        shape((rows, wide[2]), BF16),
        shape((rows, wide[3]), F32),
        shape((2, rows, 128), F32),
    ]
    names = 2 ** bits_of(chips)
    dma = pltpu.SemaphoreType.DMA
    flops = 2 * rows * width * sum(wide)
    return pl.pallas_call(
        functools.partial(project_kernel, chips),
        out_shape=gathered + made,
        in_specs=[vmem] * 8,
        out_specs=[hbm] * 9 + [vmem] * 6,
        scratch_shapes=[
            pltpu.VMEM((tokens.shape[0], width), BF16),
            pltpu.VMEM((slots, value.shape[0], value.shape[1]), BF16),
            dma((6, 2)),
            dma((6, 2)),
            dma((5, 2, names)),
            dma((5, 2, names)),
            dma((2, 4)),
            dma((2, 4)),
            dma((3,)),
        ],
        compiler_params=pltpu.CompilerParams(
            collective_id=0, has_side_effects=True, vmem_limit_bytes=60 * 2**20
        ),
        cost_estimate=pl.CostEstimate(flops=flops, bytes_accessed=60 * 2**20, transcendentals=0),
        name="gather_project",
    )(*shards, tokens, cotangent)


def reduce_kernel(chips, count, ready_count, swap_count, gains, *refs):
    refs = list(refs)

    def taken(number):
        front = refs[:number]
        del refs[:number]
        return front

    turned = taken(1)[0] if count else None
    grads, ready, swaps, gain = taken(count), taken(ready_count), taken(swap_count), taken(gains)
    results, totals, swapped_to = taken(count), taken(ready_count), taken(swap_count)
    gain_to = taken(gains)
    parts, arrived, handed = taken(count), taken(count), taken(count)
    ready_handed = taken(ready_count)
    send, recv, zsend, zrecv = taken(4)
    place = Place(chips)
    place.meet()
    bits = place.bits
    orders = [list(range(bits)), list(reversed(range(bits)))]
    back = {
        "c": place.c + (1 - place.crossed) * (1 - 2 * place.c),
        "zh": place.zh + place.crossed * (1 - 2 * place.zh),
    }

    def slot(h, mask):
        block = place.p
        for at in range(bits):
            if mask >> at & 1:
                block = flipped(block, 2 ** orders[h][at])
        return 2 * block + h

    def added(target, first, second):
        height = first.shape[0]
        step = min(64, height)

        def one(i, carry):
            at = pl.ds(pl.multiple_of(i * step, step), step)
            v = first[at, :].astype(F32) + second[at, :].astype(F32)
            target[at, :] = v.astype(target.dtype)
            return carry

        lax.fori_loop(0, height // step, one, 0)

    def hop(i, h, step, mask):
        name = mask + 2**step
        return remote(
            parts[i].at[slot(h, name)],
            arrived[i].at[h, name],
            send.at[i, h, name],
            recv.at[i, h, name],
            place.chip(orders[h][step]),
        )

    def give(i, step):
        for mask in reversed(range(2**step)):
            for h in range(2):
                hop(i, h, step, mask).start()

    def take(i, step):
        for mask in reversed(range(2**step)):
            for h in range(2):
                hop(i, h, step, mask).wait_recv()
                mine = parts[i].at[slot(h, mask)]
                added(mine, mine, arrived[i].at[h, 2**step + mask])

    def hand(i):
        if i < count:
            even, odd, to = parts[i].at[2 * place.p + 1 - place.zh], own(i), handed[i]
        else:
            even, odd, to = ready[i - count].at[1 - place.zh], own(i), ready_handed[i - count]
        moved = remote(even, to.at[0], zsend.at[i, 0], zrecv.at[i, 0], back)
        swapped = remote(odd, to.at[1], zsend.at[i, 1], zrecv.at[i, 1], place.diagonal)
        return moved, swapped

    def own(i):
        if i < count:
            return parts[i].at[2 * place.p + place.zh]
        return ready[i - count].at[place.zh]

    def hand_out(i):
        moved, swapped = hand(i)
        moved.start()
        pl.when(place.crossed == 1)(swapped.start)

    def settle(i):
        to = handed[i] if i < count else ready_handed[i - count]
        result = results[i] if i < count else totals[i - count]
        moved, swapped = hand(i)
        moved.wait_recv()

        @pl.when(place.crossed == 1)
        def _():
            swapped.wait_recv()
            added(result, to.at[0], to.at[1])

        @pl.when(place.crossed == 0)
        def _():
            added(result, to.at[0], own(i))

    def swapping(i):
        src, dst = swaps[i], swapped_to[i]
        at = count + ready_count + i
        over = remote(src, dst, zsend.at[at, 0], zrecv.at[at, 0], place.diagonal)
        return over, pltpu.make_async_copy(src, dst, zrecv.at[at, 0])

    def multiply(i):
        slots, height, _ = parts[i].shape

        def one(s, carry):
            at = pl.ds(pl.multiple_of(s * height, height), height)
            v = jnp.dot(turned[at, :], grads[i][...], preferred_element_type=F32)
            parts[i][s] = v.astype(BF16)
            return carry

        lax.fori_loop(0, slots, one, 0)

    def stage(i, at):
        if at == 0:
            multiply(i)
            give(i, bits - 1)
        elif at < bits:
            take(i, bits - at)
            give(i, bits - at - 1)
        elif at == bits:
            take(i, 0)
            hand_out(i)
        else:
            settle(i)

    for i in range(ready_count):
        hand_out(count + i)
    for i in range(swap_count):
        over, kept = swapping(i)
        pl.when(place.crossed == 1)(over.start)
        pl.when(place.crossed == 0)(kept.start)
    if gains:
        steps, landed, gsend, grecv = taken(4)
        partners = [place.high] + [place.chip(bit) for bit in range(bits)]

        def step(k):
            return remote(steps.at[k], landed.at[k], gsend.at[k], grecv.at[k], partners[k])

        over = remote(steps.at[bits + 1], gain_to[0], gsend.at[bits + 1], grecv.at[bits + 1], place.diagonal)
        kept = pltpu.make_async_copy(steps.at[bits + 1], gain_to[0], grecv.at[bits + 1])
        steps[0] = gain[0][...]
        step(0).start()
    for tick in range(count + bits + 1):
        for at in range(bits + 2):
            if 0 <= tick - at < count:
                stage(tick - at, at)
    if gains:
        for k in range(bits + 1):
            step(k).wait_recv()
            steps[k + 1] = steps[k] + landed[k]
            if k < bits:
                step(k + 1).start()
        pl.when(place.crossed == 1)(over.start)
        pl.when(place.crossed == 0)(kept.start)
    for i in range(ready_count):
        settle(count + i)
    for i in range(count):
        for h in range(2):
            for at in range(bits):
                for mask in range(2**at):
                    hop(i, h, at, mask).wait_send()
    for i in range(count + ready_count):
        moved, swapped = hand(i)
        moved.wait_send()
        pl.when(place.crossed == 1)(swapped.wait_send)
    if gains:
        for k in range(bits + 1):
            step(k).wait_send()
        pl.when(place.crossed == 1)(over.wait)
        pl.when(place.crossed == 0)(kept.wait)
    for i in range(swap_count):
        over, kept = swapping(i)
        pl.when(place.crossed == 1)(over.wait)
        pl.when(place.crossed == 0)(kept.wait)


def reduce_gradients(chips, identity, turned, grads, ready=(), swaps=(), gain=()):
    count = len(grads)
    slots = 2 * chips
    vmem = pl.BlockSpec(memory_space=pltpu.VMEM)
    wide = [g.shape[1] for g in grads]
    inputs = ([turned] if count else []) + [*grads, *ready, *swaps, *gain]
    height = turned.shape[0] // slots
    named = max(count, 1)
    shape = jax.ShapeDtypeStruct
    dma = pltpu.SemaphoreType.DMA
    moves = count + len(ready) + len(swaps)
    hops = bits_of(chips) + 2
    extra = []
    if gain:
        extra = [pltpu.VMEM((hops, *gain[0].shape), F32)] * 2 + [dma((hops,)), dma((hops,))]
    results = pl.pallas_call(
        functools.partial(reduce_kernel, chips, count, len(ready), len(swaps), len(gain)),
        out_shape=[shape((height, w), F32) for w in wide]
        + [shape(r.shape[1:], F32) for r in ready]
        + [shape(v.shape, v.dtype) for v in (*swaps, *gain)],
        in_specs=[vmem] * len(inputs),
        out_specs=[vmem] * (moves + len(gain)),
        scratch_shapes=[pltpu.VMEM((slots, height, w), BF16) for w in wide]
        + [pltpu.VMEM((2, chips, height, w), BF16) for w in wide]
        + [pltpu.VMEM((2, height, w), BF16) for w in wide]
        + [pltpu.VMEM(r.shape, BF16) for r in ready]
        + [dma((named, 2, chips)), dma((named, 2, chips)), dma((moves, 2)), dma((moves, 2))]
        + extra,
        compiler_params=pltpu.CompilerParams(
            collective_id=identity, has_side_effects=True, vmem_limit_bytes=60 * 2**20
        ),
        cost_estimate=pl.CostEstimate(
            flops=2 * turned.size * sum(wide), bytes_accessed=60 * 2**20, transcendentals=0
        ),
        name=f"reduce_gradients_{identity}",
    )(*inputs)
    return results


def swap(v):
    return lax.ppermute(v, ("c", "zh"), SWAP)


def ordered(first, second, flag, axis):
    return jnp.where(
        flag == 0,
        jnp.concatenate([first, second], axis),
        jnp.concatenate([second, first], axis),
    )


def gather_group(v, fill=()):
    far, fill = lax.optimization_barrier((lax.ppermute(v, "zl", FLIP), fill))
    near = ordered(v, far, lax.axis_index("zl"), 1)
    return ordered(near, lax.ppermute(near, "c", FLIP), lax.axis_index("c"), 1), fill


def half(v, which):
    size = v.shape[1] // 2
    return lax.dynamic_slice_in_dim(v, which * size, size, 1)


def scatter_group(v, fill=()):
    c, zl = lax.axis_index("c"), lax.axis_index("zl")
    far = lax.ppermute(half(v, 1 - c).astype(BF16), "c", FLIP)
    v = half(v, c) + far.astype(F32)
    far = lax.ppermute(half(v, 1 - zl).astype(BF16), "zl", FLIP)
    far, fill = lax.optimization_barrier((far, fill))
    return half(v, zl) + far.astype(F32), fill


def sum_group(v):
    v = v + lax.ppermute(v, "c", FLIP)
    return v + lax.ppermute(v, "zl", FLIP)


def gather_weight(w, axis):
    moved = lax.ppermute(w, ("c", "zh"), MOVE)
    swapped = swap(w)
    pair = ordered(swapped, moved, lax.axis_index("zh"), axis)
    return lax.all_gather(pair, "p", axis=axis, tiled=True)


def scatter_chips(g):
    part = lax.psum_scatter(g, "p", scatter_dimension=0, tiled=True)
    return part.reshape(2, -1, part.shape[1])


def group_norm(values):
    mean, scale = moments(values)
    return (values - mean) * scale


def gelu_tanh(values):
    return jax.nn.gelu(values, approximate=True)


def gated(gate_pre, grouped):
    return jax.nn.silu(gate_pre) * grouped


def decay_weights(running):
    span = running.shape[1]
    gap = running[:, :, None] - running[:, None, :]
    lower = jnp.arange(span)[:, None] >= jnp.arange(span)[None, :]
    return jnp.where(lower[None], jnp.exp(jnp.minimum(gap, 0.0)), 0.0)


def dot(a, b, dims):
    return lax.dot_general(a, b, (dims, ((), ())), preferred_element_type=F32)


def norm_back(d, low, mean, scale, gain, width):
    hat = (low.astype(F32) - mean) * scale
    scaled = d * gain
    sums = sum_group(jnp.stack([jnp.sum(scaled, 1), jnp.sum(scaled * hat, 1)])) / width
    d_in = scale * (scaled - sums[0][:, None] - hat * sums[1][:, None])
    return d_in, jnp.sum(d * hat, 0)


def on_device(
    tokens,
    gain_attn,
    gain_ffn,
    w_query,
    w_key,
    w_value,
    w_gate,
    w_out,
    w_up,
    w_down,
    log_decay,
    cotangent,
):
    rows = tokens.shape[0]
    heads = log_decay.shape[0]
    cols = tokens.shape[1]
    block = 2 * lax.axis_index("p") + lax.axis_index("zh")
    blocks = 2 * lax.axis_size("p")

    extra = jnp.stack([gain_attn, gain_ffn])
    tokens = jnp.concatenate([tokens, jnp.pad(extra, ((0, 14), (0, 0)))])
    decay = jnp.pad(log_decay, ((0, 8 - heads), (0, 0)))
    gathered = gather_and_project(
        blocks // 2, decay, w_query, w_key, w_value, w_gate, w_out.T, tokens, cotangent
    )
    full_decay, full_query, full_key, full_value, full_gate, full_out = gathered[:6]
    grad_full, tokens_own, gains, normed, query_rows = gathered[6:11]
    key_rows, value_rows, gate_pre, stats = gathered[11:]
    quarter = 2 * lax.axis_index("c") + lax.axis_index("zl")
    grad_own = lax.dynamic_slice_in_dim(grad_full, quarter * cols, cols, 1)
    full_query, full_key, full_value, full_gate, full_out = (
        f.reshape(-1, f.shape[2]) for f in (full_query, full_key, full_value, full_gate, full_out)
    )
    full_out = lax.all_gather(full_out, "p", axis=0, tiled=True)
    full_up = gather_weight(w_up, 0)
    full_down = gather_weight(w_down.T, 0)
    width = normed.shape[1]
    key_width = full_query.shape[1] // heads
    value_width = full_value.shape[1] // heads
    gain_two = gains[1].astype(F32)
    gain_one_own, gain_two_own = tokens_own[rows].astype(F32), tokens_own[rows + 1].astype(F32)
    tokens_own = tokens_own[:rows]
    mean_one, scale_one = stats[0, :, :1], stats[1, :, :1]
    block_sums = jnp.sum(full_decay[:, :heads], axis=2)
    log_decay = lax.dynamic_index_in_dim(full_decay, block, 0, False)[:heads]

    nn = ((1,), (0,))
    nt = ((1,), (1,))
    tn = ((0,), (0,))
    query_rows = query_rows.reshape(rows, heads, key_width)
    key_rows = key_rows.reshape(rows, heads, key_width)
    value_rows = value_rows.reshape(rows, heads, value_width)
    running = jnp.cumsum(log_decay, axis=1)
    block_decay = running[:, -1]
    query_scale = jnp.exp(running).T[:, :, None]
    key_scale = jnp.exp(block_decay[:, None] - running).T[:, :, None]
    key_decay = (key_rows * key_scale).astype(BF16)
    query_decay = (query_rows * query_scale).astype(BF16)

    def einsum(spec, a, b):
        return jnp.einsum(spec, a, b, preferred_element_type=F32)

    place = jnp.arange(blocks)[:, None]

    def decay_over(first, last):
        inside = (place >= first) & (place < last)
        return jnp.exp(jnp.sum(jnp.where(inside, block_sums, 0.0), axis=0))[:, None, None]

    def exchanged(v, stride):
        if stride == 1:
            return lax.ppermute(v, "zh", FLIP)
        pairs = [(i, i ^ (stride // 2)) for i in range(blocks // 2)]
        return lax.ppermute(v, "p", pairs)

    def carried(part, backward, fill=(), late=()):
        total, carry = part, jnp.zeros_like(part)
        stride = 1
        while stride < blocks:
            middle = block // (2 * stride) * (2 * stride) + stride
            high = block >= middle
            low_decay = decay_over(middle - stride, middle)
            high_decay = decay_over(middle, middle + stride)
            other = exchanged(total.astype(BF16), stride)
            if stride == 1:
                other, fill = lax.optimization_barrier((other, fill))
            else:
                other, late = lax.optimization_barrier((other, late))
            other = other.astype(F32)
            if backward:
                carry = jnp.where(high, carry, carry + decay_over(block + 1, middle) * other)
                total = jnp.where(high, other + low_decay * total, total + low_decay * other)
            else:
                carry = jnp.where(high, carry + decay_over(middle, block) * other, carry)
                total = jnp.where(high, high_decay * other + total, high_decay * total + other)
            stride *= 2
        return carry.astype(BF16), fill, late

    state, _, _ = carried(einsum("nhd,nhe->hde", key_decay, value_rows), False)
    decays = decay_weights(running)
    weighted = (einsum("nhd,mhd->hnm", query_rows, key_rows) * decays).astype(BF16)
    retained = einsum("hnm,mhe->hne", weighted, value_rows) + einsum(
        "nhd,hde->hne", query_decay, state
    )
    grouped = group_norm(retained)
    grouped = jnp.concatenate([grouped[h] for h in range(heads)], 1)
    mixed_rows = gated(gate_pre, grouped).astype(BF16)
    attended, turned = scatter_group(dot(mixed_rows, full_out, nt), normed.T)
    hidden = tokens_own.astype(F32) + attended
    hidden_own = hidden.astype(BF16)
    hidden_full, d_act = gather_group(hidden_own, dot(grad_full, full_down, nn))
    hidden_full = hidden_full.astype(F32)
    mean_two, scale_two = moments(hidden_full)
    normed_ffn = ((hidden_full - mean_two) * scale_two * gain_two).astype(BF16)
    pre_act = dot(normed_ffn, full_up, nn)
    activated, gelu_back = jax.vjp(gelu_tanh, pre_act)
    activated = activated.astype(BF16)
    d_pre = gelu_back(d_act)[0].astype(BF16)
    d_normed_ffn, grad_down = scatter_group(
        dot(d_pre, full_up, nt), dot(grad_full, activated, tn).astype(BF16)
    )
    part_down = scatter_chips(grad_down)
    d_hidden_norm, d_gain_two = norm_back(
        d_normed_ffn, hidden_own, mean_two, scale_two, gain_two_own, width
    )
    d_hidden = grad_own.astype(F32) + d_hidden_norm
    d_attended, grad_up = gather_group(
        d_hidden.astype(BF16), dot(normed_ffn, d_pre, tn).astype(BF16)
    )
    part_up = scatter_chips(grad_up)
    d_mixed = dot(d_attended, full_out, nn)
    _, gate_back = jax.vjp(gated, gate_pre, grouped)
    d_gate, d_grouped = gate_back(d_mixed)
    d_gate = d_gate.astype(BF16)
    _, group_back = jax.vjp(group_norm, retained)
    d_grouped = jnp.stack(
        [d_grouped[:, h * value_width : (h + 1) * value_width] for h in range(heads)]
    )
    ffn, d_retained = scatter_group(
        dot(activated, full_down, nt), group_back(d_grouped)[0].astype(BF16)
    )
    output = swap((hidden + ffn).astype(BF16))
    later_grad, grad_out, output = carried(
        einsum("nhd,hne->hde", query_decay, d_retained),
        True,
        dot(d_attended, mixed_rows, tn).astype(BF16),
        output,
    )
    part_out = scatter_chips(grad_out)
    d_raw = (einsum("hne,mhe->hnm", d_retained, value_rows) * decays).astype(BF16)
    d_query = (
        einsum("hnm,mhd->nhd", d_raw, key_rows)
        + einsum("hne,hde->nhd", d_retained, state) * query_scale
    )
    d_query = d_query.astype(BF16).reshape(rows, heads * key_width)
    d_keys = (
        einsum("hnm,nhd->mhd", d_raw, query_rows)
        + einsum("mhe,hde->mhd", value_rows, later_grad) * key_scale
    )
    d_keys = d_keys.astype(BF16).reshape(rows, heads * key_width)
    d_values = einsum("hnm,hne->mhe", weighted, d_retained) + einsum(
        "mhd,hde->mhe", key_decay, later_grad
    )
    d_values = d_values.astype(BF16).reshape(rows, heads * value_width)
    d_normed, first = scatter_group(
        dot(d_gate, full_gate, nt)
        + dot(d_query, full_query, nt)
        + dot(d_keys, full_key, nt)
        + dot(d_values, full_value, nt),
        reduce_gradients(
            blocks // 2, 1, turned, (d_query, d_values, d_gate, d_keys),
            (part_down, part_up, part_out),
        ),
    )
    grad_query, grad_value, grad_gate, grad_key, grad_down, grad_up, grad_out = first
    d_tokens_norm, d_gain_one = norm_back(
        d_normed, tokens_own, mean_one, scale_one, gain_one_own, width
    )
    input_grad = (d_hidden + d_tokens_norm).astype(BF16)
    gain = jnp.concatenate([d_gain_one[None], d_gain_two[None], jnp.zeros((6, cols), F32)])
    input_grad, gain = reduce_gradients(blocks // 2, 2, turned, (), (), (input_grad,), (gain,))
    return (
        output,
        input_grad.astype(F32),
        gain[0],
        gain[1],
        grad_query,
        grad_key,
        grad_value,
        grad_gate,
        grad_out.T,
        grad_up,
        grad_down.T,
    )


def solution(mesh):
    seq, head = mesh.devices.shape
    finer = Mesh(mesh.devices.reshape(seq // 2, 2, head // 2, 2), ("p", "c", "zh", "zl"))
    seq, head = ("p", "c"), ("zh", "zl")
    by_row, by_column, one = P(seq, head), P(head, seq), P(head)
    in_specs = (
        (by_row, one, one) + (by_row,) * 4 + (by_column, by_row, by_column) + (by_column, by_row)
    )
    out_specs = (by_row, by_row, one, one) + (by_row,) * 4 + (by_column, by_row, by_column)
    return jax.shard_map(
        on_device, mesh=finer, in_specs=in_specs, out_specs=out_specs, check_vma=False
    )
```
